32 devices in a mesh: dp: 1 (over z), sp: 4 (over y), tp: 8 (over x, core).
Axes of the slice: x: 4, y: 4, z: 1, core: 2. Of those that a mesh axis runs over, the one named last changes fastest.
The devices are a block of a 4x4x8 slice.
Arguments:
- hidden_in: bfloat16 [4096, 3072], P(('dp', 'sp', 'tp'))
- segment_ids: int32 [4096], P(('dp', 'sp', 'tp'))
- positions: int32 [4096], P(('dp', 'sp', 'tp'))
- attn_gain: bfloat16 [4, 3072], replicated
- w_q: bfloat16 [4, 3072, 3072], P(None, None, 'tp')
- w_k: bfloat16 [4, 3072, 1024], P(None, None, 'tp')
- w_v: bfloat16 [4, 3072, 1024], P(None, None, 'tp')
- w_o: bfloat16 [4, 3072, 3072], P(None, 'tp')
- mlp_gain: bfloat16 [4, 3072], replicated
- w_gate: bfloat16 [4, 3072, 8192], P(None, None, 'tp')
- w_up: bfloat16 [4, 3072, 8192], P(None, None, 'tp')
- w_down: bfloat16 [4, 8192, 3072], P(None, 'tp')
Outputs:
- output 1: bfloat16 [4096, 3072], P(('dp', 'sp', 'tp'))
- output 2: bfloat16 [4, 4096, 8, 128], P(None, ('dp', 'sp'), 'tp')
- output 3: bfloat16 [4, 4096, 8, 128], P(None, ('dp', 'sp'), 'tp')
All inputs are finite; a program needn't handle non-finite values.
Results may differ from the reference program's by a relative error of at most 0.02.
Values are sent between devices in bfloat16 or wider.
A program may use at most 768 MiB of HBM per device.

```python
import math
import jax
import jax.numpy as jnp
from jax import lax

TOKENS = 4096
MODEL_DIM = 3072
HEADS = 24
KV_HEADS = 8
HEAD_DIM = 128
FFN_DIM = 8192
LAYERS = 4
SEGMENTS = 4

GROUP = HEADS // KV_HEADS
Q_BLOCK = math.gcd(TOKENS, 32)
ROPE_BASE = 1e4
NORM_EPS = 1e-5
SCORE_SCALE = HEAD_DIM ** -0.5


def setup_inputs(seed: int = 0, part: int = 0) -> dict:
    part_key = jax.random.fold_in(jax.random.key(seed), part)
    act_keys = jax.random.split(part_key, 6)
    base_noise = jax.random.normal(act_keys[0], (TOKENS, MODEL_DIM), jnp.float32)
    cycles = jax.random.uniform(act_keys[1], (MODEL_DIM,), jnp.float32, 0.5, 3.0)
    phases = jax.random.uniform(act_keys[2], (MODEL_DIM,), jnp.float32, 0.0, 6.2832)
    time_ramp = jnp.arange(TOKENS, dtype=jnp.float32) / TOKENS
    drift_part = jnp.cos(6.2832 * time_ramp[:, None] * cycles[None, :] + phases[None, :])
    hidden_in = (0.6 * base_noise + 1.2 * drift_part).astype(jnp.bfloat16)
    cut_points = jax.random.permutation(act_keys[3], TOKENS - 1)[: SEGMENTS - 1] + 1
    seg_marks = jnp.zeros((TOKENS,), jnp.int32).at[cut_points].set(1)
    segment_ids = jnp.cumsum(seg_marks).astype(jnp.int32)
    pos_steps = jax.random.randint(act_keys[4], (TOKENS,), 1, 3)
    pos_start = jax.random.randint(act_keys[5], (), 0, 64)
    positions = (jnp.cumsum(pos_steps) + pos_start).astype(jnp.int32)
    w_keys = jax.random.split(jax.random.key(seed + 1), 9)

    def normal_w(key_w, shape_w, scale_w):
        return (jax.random.normal(key_w, shape_w, jnp.float32) * scale_w).astype(jnp.bfloat16)

    def gain_w(key_w):
        return (1.0 + 0.3 * jax.random.normal(key_w, (LAYERS, MODEL_DIM), jnp.float32)).astype(jnp.bfloat16)

    dim_scale = MODEL_DIM ** -0.5
    return {
        'hidden_in': hidden_in,
        'segment_ids': segment_ids,
        'positions': positions,
        'attn_gain': gain_w(w_keys[0]),
        'w_q': normal_w(w_keys[1], (LAYERS, MODEL_DIM, HEADS * HEAD_DIM), 1.4 * dim_scale),
        'w_k': normal_w(w_keys[2], (LAYERS, MODEL_DIM, KV_HEADS * HEAD_DIM), 1.4 * dim_scale),
        'w_v': normal_w(w_keys[3], (LAYERS, MODEL_DIM, KV_HEADS * HEAD_DIM), dim_scale),
        'w_o': normal_w(w_keys[4], (LAYERS, HEADS * HEAD_DIM, MODEL_DIM), 0.7 * (HEADS * HEAD_DIM) ** -0.5),
        'mlp_gain': gain_w(w_keys[5]),
        'w_gate': normal_w(w_keys[6], (LAYERS, MODEL_DIM, FFN_DIM), dim_scale),
        'w_up': normal_w(w_keys[7], (LAYERS, MODEL_DIM, FFN_DIM), dim_scale),
        'w_down': normal_w(w_keys[8], (LAYERS, FFN_DIM, MODEL_DIM), 0.7 * FFN_DIM ** -0.5),
    }


def rms_norm(hidden, gain_vec):
    hidden32 = hidden.astype(jnp.float32)
    inv_rms = lax.rsqrt(jnp.mean(hidden32 * hidden32, axis=-1, keepdims=True) + NORM_EPS)
    return (hidden32 * inv_rms * gain_vec.astype(jnp.float32)).astype(jnp.bfloat16)


def rotary(rot_in, positions):
    half_dim = HEAD_DIM // 2
    inv_freq = ROPE_BASE ** (-jnp.arange(half_dim, dtype=jnp.float32) / half_dim)
    angles = positions.astype(jnp.float32)[..., None] * inv_freq
    cos_val = jnp.cos(angles)[..., None, :]
    sin_val = jnp.sin(angles)[..., None, :]
    first_half = rot_in[..., :half_dim]
    second_half = rot_in[..., half_dim:]
    return jnp.concatenate([first_half * cos_val - second_half * sin_val, second_half * cos_val + first_half * sin_val], axis=-1)


def attention(q_rot, k_rot, v_val, segment_ids):
    n_blocks = TOKENS // Q_BLOCK
    key_index = jnp.arange(TOKENS)
    k_wide = k_rot.astype(jnp.float32)
    v_wide = v_val.astype(jnp.float32)

    def one_block(block_in):
        q_blk, idx_blk, seg_blk = block_in
        scores = jnp.einsum('qkgd,skd->kgqs', q_blk.astype(jnp.float32), k_wide) * SCORE_SCALE
        allowed = (idx_blk[:, None] >= key_index[None, :]) & (seg_blk[:, None] == segment_ids[None, :])
        probs = jax.nn.softmax(jnp.where(allowed, scores, -1e30), axis=-1).astype(jnp.bfloat16)
        return jnp.einsum('kgqs,skd->qkgd', probs.astype(jnp.float32), v_wide).astype(jnp.bfloat16)

    blocks = (q_rot.reshape(n_blocks, Q_BLOCK, KV_HEADS, GROUP, HEAD_DIM),
              key_index.reshape(n_blocks, Q_BLOCK), segment_ids.reshape(n_blocks, Q_BLOCK))
    return lax.map(one_block, blocks).reshape(TOKENS, HEADS * HEAD_DIM)


def reference(hidden_in, segment_ids, positions, attn_gain, w_q, w_k, w_v, w_o, mlp_gain, w_gate, w_up, w_down):
    def layer_step(hidden, layer_w):
        gain_attn, wq_l, wk_l, wv_l, wo_l, gain_mlp, wg_l, wu_l, wd_l = layer_w
        normed = rms_norm(hidden, gain_attn)
        q_lin = jnp.dot(normed, wq_l, preferred_element_type=jnp.float32).reshape(TOKENS, HEADS, HEAD_DIM)
        k_lin = jnp.dot(normed, wk_l, preferred_element_type=jnp.float32).reshape(TOKENS, KV_HEADS, HEAD_DIM)
        v_val = jnp.dot(normed, wv_l, preferred_element_type=jnp.float32).astype(jnp.bfloat16).reshape(TOKENS, KV_HEADS, HEAD_DIM)
        q_rot = rotary(q_lin, positions).astype(jnp.bfloat16).reshape(TOKENS, KV_HEADS, GROUP, HEAD_DIM)
        k_rot = rotary(k_lin, positions).astype(jnp.bfloat16)
        att_out = attention(q_rot, k_rot, v_val, segment_ids)
        proj_out = jnp.dot(att_out, wo_l, preferred_element_type=jnp.float32).astype(jnp.bfloat16)
        hidden_mid = (hidden.astype(jnp.float32) + proj_out.astype(jnp.float32)).astype(jnp.bfloat16)
        normed_mlp = rms_norm(hidden_mid, gain_mlp)
        gate_lin = jnp.dot(normed_mlp, wg_l, preferred_element_type=jnp.float32)
        up_lin = jnp.dot(normed_mlp, wu_l, preferred_element_type=jnp.float32)
        act_vals = (jax.nn.silu(gate_lin) * up_lin).astype(jnp.bfloat16)
        down_out = jnp.dot(act_vals, wd_l, preferred_element_type=jnp.float32).astype(jnp.bfloat16)
        hidden_new = (hidden_mid.astype(jnp.float32) + down_out.astype(jnp.float32)).astype(jnp.bfloat16)
        return hidden_new, (k_rot, v_val)

    hidden_out, caches = lax.scan(layer_step, hidden_in, (attn_gain, w_q, w_k, w_v, w_o, mlp_gain, w_gate, w_up, w_down))
    return hidden_out, caches[0], caches[1]
```

```python
import jax
import jax.numpy as jnp
from jax import lax
from jax.experimental import pallas as pl
from jax.experimental.pallas import tpu as pltpu
from jax.sharding import PartitionSpec as P

HEAD_DIM = 128
ROPE_BASE = 1e4
NORM_EPS = 1e-5
LOG2E = 1.4426950408889634
SCORE_EXP2 = HEAD_DIM ** -0.5 * LOG2E
NEG = -1e30
MESH = pl.DeviceIdType.MESH
F32 = jnp.float32
BF16 = jnp.bfloat16
CORES = 2
BATCHES = 2
OPP, RIGHT, LEFT, OWN = 0, 1, 2, 3


def dot(a, b):
    return jnp.dot(a, b, preferred_element_type=F32)


def make_kernel(n_layers, n_sp, n_tp, sub, model_dim, q_dim, ffn, col):
    chips = n_tp // CORES
    half = sub // 2
    unit = CORES * sub
    heads = q_dim // HEAD_DIM
    chip_rows = BATCHES * unit
    n_pair = chips // 2

    def kernel(hid, cos_t, sin_t, q_seg, k_seg, own_seg, gain_a, gain_m, wq_h, wk_h, wv_h, wo_h, wg_h, wu_h, wd_h,
               out, k_out, v_out,
               res, gath, part, acc_rs, opp_in, nb_in, act, q_buf, m_buf, l_buf, o_buf, kv,
               w_qkv, w_o, w_g, w_u, w_d,
               w_sem, ag_send, ag_sib, ag_l, ag_r, ag_o, ag_sf, rs_dsend, rs_sib, rs_send, rs_opp, rs_nb, kv_send, kv_recv, c_sem):
        y = lax.axis_index('sp')
        me = lax.axis_index('tp')
        x = me // CORES
        c = lax.rem(me, CORES)
        oc = 1 - c
        xl = lax.rem(x + chips - 1, chips)
        xr = lax.rem(x + 1, chips)
        xo = lax.rem(x + 2, chips)
        unit_of = {OPP: xo, RIGHT: xr, LEFT: xl, OWN: x}
        sib = {'tp': x * CORES + oc}
        right = {'tp': xr * CORES + c}
        left = {'tp': xl * CORES + c}
        lo = pl.ds(0, half)
        hi = pl.ds(half, half)

        def rdma(src, dst, ssem, rsem, dev):
            return pltpu.make_async_remote_copy(src_ref=src, dst_ref=dst, send_sem=ssem, recv_sem=rsem,
                                                device_id=dev, device_id_type=MESH)

        def attn_weights(l):
            return [pltpu.make_async_copy(wq_h.at[l], w_qkv.at[:, pl.ds(0, q_dim)], w_sem.at[0]),
                    pltpu.make_async_copy(wk_h.at[l], w_qkv.at[:, pl.ds(q_dim, HEAD_DIM)], w_sem.at[1]),
                    pltpu.make_async_copy(wv_h.at[l], w_qkv.at[:, pl.ds(q_dim + HEAD_DIM, HEAD_DIM)], w_sem.at[2]),
                    pltpu.make_async_copy(wo_h.at[l], w_o, w_sem.at[3])]

        def mlp_weights(l):
            return [pltpu.make_async_copy(wg_h.at[l], w_g, w_sem.at[4]),
                    pltpu.make_async_copy(wu_h.at[l], w_u, w_sem.at[5]),
                    pltpu.make_async_copy(wd_h.at[l], w_d, w_sem.at[6])]

        for cp in attn_weights(0) + mlp_weights(0):
            cp.start()

        barrier = pltpu.get_barrier_semaphore()
        for dev in (sib, right, left):
            pl.semaphore_signal(barrier, inc=1, device_id=dev, device_id_type=MESH)
        for d in range(1, n_sp):
            pl.semaphore_signal(barrier, inc=1, device_id={'sp': lax.rem(y + d, n_sp)}, device_id_type=MESH)
        pl.semaphore_wait(barrier, 3 + n_sp - 1)

        def ag_copies(b):
            own = gath.at[b, x, c]
            return {
                'sib': rdma(own, own, ag_send.at[b, 0], ag_sib.at[b], sib),
                'r_lo': rdma(own.at[lo], own.at[lo], ag_send.at[b, 1], ag_l.at[b, 0], right),
                'l_hi': rdma(own.at[hi], own.at[hi], ag_send.at[b, 2], ag_r.at[b, 1], left),
                'r_hi': rdma(own.at[hi], own.at[hi], ag_send.at[b, 3], ag_l.at[b, 1], right),
                'l_lo': rdma(own.at[lo], own.at[lo], ag_send.at[b, 4], ag_r.at[b, 0], left),
                'f_r': rdma(gath.at[b, xl, c, lo], gath.at[b, xl, c, lo], ag_send.at[b, 5], ag_o.at[b, 0], right),
                'f_l': rdma(gath.at[b, xr, c, hi], gath.at[b, xr, c, hi], ag_send.at[b, 6], ag_o.at[b, 1], left),
                's_l': rdma(gath.at[b, xl, c], gath.at[b, xl, c], ag_send.at[b, 7], ag_sf.at[b, LEFT], sib),
                's_r': rdma(gath.at[b, xr, c], gath.at[b, xr, c], ag_send.at[b, 8], ag_sf.at[b, RIGHT], sib),
                's_o': rdma(gath.at[b, xo, c], gath.at[b, xo, c], ag_send.at[b, 9], ag_sf.at[b, OPP], sib),
            }

        def arrived(ref, sem):
            rdma(ref, ref, ag_send.at[0, 0], sem, sib).wait_recv()

        def ag0a(b):
            cps = ag_copies(b)
            for name in ('sib', 'r_lo', 'l_hi'):
                cps[name].start()

        def ag0b(b):
            cps = ag_copies(b)
            for name in ('r_hi', 'l_lo'):
                cps[name].start()

        def ag1(b):
            cps = ag_copies(b)
            arrived(gath.at[b, xl, c, lo], ag_l.at[b, 0])
            cps['f_r'].start()
            arrived(gath.at[b, xr, c, hi], ag_r.at[b, 1])
            cps['f_l'].start()

        def ag2(b):
            cps = ag_copies(b)
            arrived(gath.at[b, xl, c, hi], ag_l.at[b, 1])
            cps['s_l'].start()
            arrived(gath.at[b, xr, c, lo], ag_r.at[b, 0])
            cps['s_r'].start()

        def ag3(b):
            cps = ag_copies(b)
            arrived(gath.at[b, xo, c, lo], ag_o.at[b, 0])
            arrived(gath.at[b, xo, c, hi], ag_o.at[b, 1])
            cps['s_o'].start()

        def ag_unit_ready(b, k):
            arrived(gath.at[b, unit_of[k], oc], ag_sib.at[b] if k == OWN else ag_sf.at[b, k])

        def ag_sent(b):
            for cp in ag_copies(b).values():
                cp.wait_send()

        def rs_pair(b, k):
            return rdma(part.at[k, oc], acc_rs.at[b, k], rs_dsend.at[b, k], rs_sib.at[b, k], sib)

        def rs_copies(b):
            return {
                'o_r': rdma(acc_rs.at[b, OPP, lo], opp_in.at[b, 0], rs_send.at[b, 0], rs_opp.at[b, 0], right),
                'o_l': rdma(acc_rs.at[b, OPP, hi], opp_in.at[b, 1], rs_send.at[b, 1], rs_opp.at[b, 1], left),
                'r_hi': rdma(acc_rs.at[b, RIGHT, hi], nb_in.at[b, 0, hi], rs_send.at[b, 2], rs_nb.at[b, 0, 1], right),
                'l_lo': rdma(acc_rs.at[b, LEFT, lo], nb_in.at[b, 1, lo], rs_send.at[b, 3], rs_nb.at[b, 1, 0], left),
                'r_lo': rdma(acc_rs.at[b, RIGHT, lo], nb_in.at[b, 0, lo], rs_send.at[b, 4], rs_nb.at[b, 0, 0], right),
                'l_hi': rdma(acc_rs.at[b, LEFT, hi], nb_in.at[b, 1, hi], rs_send.at[b, 5], rs_nb.at[b, 1, 1], left),
            }

        def pair_sum(b, k):
            cp = rs_pair(b, k)
            cp.wait_send()
            cp.wait_recv()
            acc_rs[b, k] = (acc_rs[b, k].astype(F32) + part[k, c].astype(F32)).astype(BF16)

        def rs1(b):
            pair_sum(b, OPP)
            cps = rs_copies(b)
            cps['o_r'].start()
            cps['o_l'].start()

        def rs2a(b):
            cps = rs_copies(b)
            pair_sum(b, RIGHT)
            cps['r_hi'].start()
            pair_sum(b, LEFT)
            cps['l_lo'].start()
            pair_sum(b, OWN)

        def rs2b(b):
            cps = rs_copies(b)
            cps['o_r'].wait_recv()
            acc_rs[b, RIGHT, lo] = (acc_rs[b, RIGHT, lo].astype(F32) + opp_in[b, 0].astype(F32)).astype(BF16)
            cps['r_lo'].start()
            cps['o_l'].wait_recv()
            acc_rs[b, LEFT, hi] = (acc_rs[b, LEFT, hi].astype(F32) + opp_in[b, 1].astype(F32)).astype(BF16)
            cps['l_hi'].start()

        def fin(b):
            cps = rs_copies(b)
            for name in ('r_hi', 'l_lo', 'r_lo', 'l_hi'):
                cps[name].wait_recv()
            for cp in cps.values():
                cp.wait_send()
            total = (acc_rs[b, OWN].astype(F32) + nb_in[b, 0].astype(F32) + nb_in[b, 1].astype(F32)).astype(BF16)
            res[b] = (res[b].astype(F32) + total.astype(F32)).astype(BF16)

        def norm(b, gain):
            h = res[b].astype(F32)
            inv = lax.rsqrt(jnp.mean(h * h, axis=-1, keepdims=True) + NORM_EPS)
            gath[b, x, c] = (h * inv * gain).astype(BF16)

        def store_part(k, lhs, w, n):
            cols = pl.ds(pl.multiple_of(n * col, col), col)
            r = dot(lhs, w[:, cols]).astype(BF16)
            part[k, :, :, cols] = r.reshape(CORES, sub, col)

        def rope(v, b, u):
            return v * cos_t[u, b] + pltpu.roll(v, HEAD_DIM // 2, 1) * sin_t[u, b]

        def qkv(l, b, k):
            ag_unit_ready(b, k)
            u = unit_of[k]
            n = gath[b, u].reshape(unit, model_dim)
            for h0 in range(0, heads + 2, 2):
                width = min(2, heads + 2 - h0) * HEAD_DIM
                r = dot(n, w_qkv[:, pl.ds(h0 * HEAD_DIM, width)])
                for h in range(h0, min(h0 + 2, heads + 2)):
                    v = r[:, (h - h0) * HEAD_DIM:(h - h0 + 1) * HEAD_DIM]
                    if h < heads:
                        q_buf[b, k, h] = rope(v, b, u).astype(BF16)
                    elif h == heads:
                        kv[l, y, u, b, :, :, pl.ds(0, HEAD_DIM)] = rope(v, b, u).astype(BF16).reshape(CORES, sub, HEAD_DIM)
                    else:
                        kv[l, y, u, b, :, :, pl.ds(HEAD_DIM, HEAD_DIM)] = v.astype(BF16).reshape(CORES, sub, HEAD_DIM)
            m_buf[b, k] = jnp.full(m_buf.shape[2:], NEG, F32)
            l_buf[b, k] = jnp.zeros(l_buf.shape[2:], F32)
            o_buf[b, k] = jnp.zeros(o_buf.shape[2:], F32)
            for d in range(1, n_sp):
                @pl.when(y + d < n_sp)
                def _():
                    kv_copy(l, kv.at[l, y, u, b], d).start()

        def kv_copy(l, ref, d):
            return rdma(ref, ref, kv_send.at[d - 1], kv_recv.at[l, y], {'sp': lax.min(y + d, n_sp - 1)})

        def cache_copies(l):
            cps = []
            for b in range(BATCHES):
                for core in range(CORES):
                    for i, ref in enumerate((k_out, v_out)):
                        cps.append(pltpu.make_async_copy(kv.at[l, y, :, b, core, :, pl.ds(i * HEAD_DIM, HEAD_DIM)],
                                                         ref.at[l, :, core, b], c_sem.at[b, core, i]))
            return cps

        def flash(b, k, keys, vals, mask):
            n_keys = keys.shape[0]
            q = q_buf[b, k].reshape(heads * unit, HEAD_DIM)
            s = lax.dot_general(q, keys, (((1,), (1,)), ((), ())), preferred_element_type=F32)
            s = jnp.where(mask[None], s.reshape(heads, unit, n_keys), NEG).reshape(heads * unit, n_keys)
            m_old = m_buf[b, k]
            m_new = jnp.maximum(m_old, jnp.max(s, axis=-1, keepdims=True))
            alpha = jnp.exp2((m_old - m_new) * SCORE_EXP2)
            p = jnp.exp2((s - jnp.concatenate([m_new] * (n_keys // HEAD_DIM), axis=1)) * SCORE_EXP2)
            m_buf[b, k] = m_new
            total = l_buf[b, k] * alpha
            for i in range(n_keys // HEAD_DIM):
                total = total + p[:, i * HEAD_DIM:(i + 1) * HEAD_DIM]
            l_buf[b, k] = total
            o_buf[b, k] = o_buf[b, k] * alpha + dot(p.astype(BF16), vals)

        def attn_rows_below(l, b, k, on):
            u = unit_of[k]

            def step(j, carry):
                block = kv[l, j // n_pair, pl.ds(lax.rem(j, n_pair) * 2, 2)].reshape(2 * chip_rows, 2 * HEAD_DIM)
                seg = jnp.concatenate([q_seg[u, b]] * (2 * chip_rows // HEAD_DIM), axis=1)
                mask = seg == jnp.broadcast_to(k_seg[j], (unit, 2 * chip_rows))
                flash(b, k, block[:, :HEAD_DIM], block[:, HEAD_DIM:], mask)
                return carry

            lax.fori_loop(0, jnp.where(on, y * n_pair, 0), step, 0)

        def kv_ready(l, on):
            for r in range(n_sp - 1):
                @pl.when(jnp.logical_and(on, r < y))
                def _():
                    rdma(kv.at[l, r], kv.at[l, r], kv_send.at[0], kv_recv.at[l, r], sib).wait_recv()

        def attn_own(l, b, k):
            u = unit_of[k]
            row = lax.broadcasted_iota(jnp.int32, (unit, chip_rows), 0)
            lane = lax.broadcasted_iota(jnp.int32, (unit, chip_rows), 1)
            q_tok = u * chip_rows + row // sub * (BATCHES * sub) + b * sub + lax.rem(row, sub)
            k_tok = lax.rem(lane, unit) // sub * (BATCHES * sub) + lane // unit * sub + lax.rem(lane, sub)

            def step(j, carry):
                block = kv[l, y, j].reshape(chip_rows, 2 * HEAD_DIM)
                seg = jnp.concatenate([q_seg[u, b]] * (chip_rows // HEAD_DIM), axis=1)
                mask = jnp.logical_and(seg == jnp.broadcast_to(own_seg[j], (unit, chip_rows)), q_tok >= k_tok + j * chip_rows)
                flash(b, k, block[:, :HEAD_DIM], block[:, HEAD_DIM:], mask)
                return carry

            lax.fori_loop(0, u + 1, step, 0)

        def attn_out(b, k):
            inv = 1.0 / jnp.sum(l_buf[b, k], axis=-1, keepdims=True)
            o = (o_buf[b, k] * inv).astype(BF16)
            o = jnp.concatenate([o[h * unit:(h + 1) * unit] for h in range(heads)], axis=1)

            def step(n, carry):
                store_part(k, o, w_o, n)
                return carry

            lax.fori_loop(0, model_dim // col, step, 0)
            rs_pair(b, k).start()

        ffn_col = min(256, ffn)

        def gate_up(b, k):
            ag_unit_ready(b, k)
            n = gath[b, unit_of[k]].reshape(unit, model_dim)

            def step(j, carry):
                cols = pl.ds(pl.multiple_of(j * ffn_col, ffn_col), ffn_col)
                g = dot(n, w_g[:, cols])
                act[b, k, :, cols] = (g * jax.nn.sigmoid(g) * dot(n, w_u[:, cols])).astype(BF16)
                return carry

            lax.fori_loop(0, ffn // ffn_col, step, 0)

        def down(b, k):
            def step(n, carry):
                store_part(k, act[b, k], w_d, n)
                return carry

            lax.fori_loop(0, model_dim // col, step, 0)
            rs_pair(b, k).start()

        A, B = 0, 1
        res[...] = hid[...]
        norm(A, gain_a[0])
        ag0a(A)
        ag0b(A)

        def layer(l, carry):
            more = l + 1 < n_layers
            nxt = lax.min(l + 1, n_layers - 1)
            later = l > 0
            for cp in attn_weights(l)[:3]:
                cp.wait()
            qkv(l, A, OWN)

            @pl.when(later)
            def _():
                fin(B)
            norm(B, gain_a[l])
            ag0a(B)
            ag1(A)
            ag0b(B)
            ag2(A)
            qkv(l, A, LEFT)
            qkv(l, A, RIGHT)
            kv_ready(l, later)
            attn_rows_below(l, A, OWN, later)
            ag3(A)
            qkv(l, B, OWN)
            ag1(B)
            qkv(l, A, OPP)
            attn_rows_below(l, A, LEFT, later)
            attn_rows_below(l, A, RIGHT, later)
            ag2(B)
            qkv(l, B, LEFT)
            qkv(l, B, RIGHT)
            attn_rows_below(l, A, OPP, later)
            attn_rows_below(l, B, OWN, later)
            ag3(B)
            attn_rows_below(l, B, LEFT, later)
            qkv(l, B, OPP)
            for cp in cache_copies(l):
                cp.start()
            kv_ready(l, jnp.logical_not(later))
            for k in (OPP, RIGHT, LEFT, OWN):
                attn_rows_below(l, A, k, jnp.logical_not(later))
            attn_weights(l)[3].wait()
            ag_sent(A)
            attn_own(l, A, OPP)
            attn_out(A, OPP)
            attn_own(l, A, RIGHT)
            attn_out(A, RIGHT)
            rs1(A)
            attn_own(l, A, LEFT)
            attn_out(A, LEFT)
            attn_own(l, A, OWN)
            attn_out(A, OWN)
            rs2a(A)
            ag_sent(B)
            attn_rows_below(l, B, OPP, True)
            attn_own(l, B, OPP)
            attn_out(B, OPP)
            rs2b(A)
            attn_rows_below(l, B, RIGHT, True)
            attn_own(l, B, RIGHT)
            attn_out(B, RIGHT)
            rs1(B)
            attn_rows_below(l, B, LEFT, jnp.logical_not(later))
            attn_own(l, B, LEFT)
            attn_out(B, LEFT)
            attn_rows_below(l, B, OWN, jnp.logical_not(later))
            attn_own(l, B, OWN)
            attn_out(B, OWN)

            @pl.when(more)
            def _():
                for cp in attn_weights(nxt):
                    cp.start()
            rs2a(B)
            fin(A)
            norm(A, gain_m[l])
            ag0a(A)
            rs2b(B)
            ag0b(A)

            for cp in mlp_weights(l)[:2]:
                cp.wait()
            gate_up(A, OWN)
            fin(B)
            norm(B, gain_m[l])
            ag0a(B)
            ag1(A)
            ag0b(B)
            ag2(A)
            gate_up(A, LEFT)
            gate_up(A, RIGHT)
            ag3(A)
            gate_up(B, OWN)
            ag1(B)
            gate_up(A, OPP)
            mlp_weights(l)[2].wait()
            ag_sent(A)
            down(A, OPP)
            down(A, RIGHT)
            rs1(A)
            down(A, LEFT)
            down(A, OWN)
            ag2(B)
            rs2a(A)
            gate_up(B, LEFT)
            gate_up(B, RIGHT)
            ag3(B)
            gate_up(B, OPP)
            ag_sent(B)
            down(B, OPP)
            down(B, RIGHT)
            rs2b(A)
            rs1(B)
            down(B, LEFT)
            down(B, OWN)

            @pl.when(more)
            def _():
                for cp in mlp_weights(nxt):
                    cp.start()
            rs2a(B)
            fin(A)

            @pl.when(more)
            def _():
                norm(A, gain_a[nxt])
                ag0a(A)
            rs2b(B)

            @pl.when(more)
            def _():
                ag0b(A)
            for cp in cache_copies(l):
                cp.wait()
            for d in range(1, n_sp):
                @pl.when(y + d < n_sp)
                def _():
                    kv_copy(l, kv.at[l, y], d).wait_send()
            return carry

        lax.fori_loop(0, n_layers, layer, 0)
        fin(B)
        out[...] = res[...]

    return kernel


def solution(mesh):
    n_sp, n_tp = mesh.shape['sp'], mesh.shape['tp']
    chips = n_tp // CORES
    tok_spec = P(('dp', 'sp', 'tp'))
    col_spec = P(None, None, 'tp')
    row_spec = P(None, 'tp', None)
    cache_spec = P(None, ('dp', 'sp'), 'tp', None)

    def device_fn(hidden_in, segment_ids, positions, attn_gain, w_q, w_k, w_v, w_o, mlp_gain, w_gate, w_up, w_down):
        tok_local, model_dim = hidden_in.shape
        n_layers, _, q_dim = w_q.shape
        ffn = w_gate.shape[2]
        sub = tok_local // BATCHES
        unit = CORES * sub
        n_rows = tok_local * n_tp
        heads = q_dim // HEAD_DIM
        col = min(512, model_dim)

        marks = lax.all_gather(jnp.stack([segment_ids, positions]), ('sp', 'tp'))
        marks = marks.reshape(n_sp, chips, CORES, 2, BATCHES, sub).transpose(3, 0, 1, 4, 2, 5)
        segs = marks[0]
        row = lax.axis_index('sp')
        own_seg = lax.dynamic_index_in_dim(segs, row, 0, False)
        own_pos = lax.dynamic_index_in_dim(marks[1], row, 0, False)
        half_dim = HEAD_DIM // 2
        inv_freq = ROPE_BASE ** (-jnp.arange(half_dim, dtype=F32) / half_dim)
        angles = own_pos.reshape(chips, BATCHES, unit, 1).astype(F32) * inv_freq
        cos_v, sin_v = jnp.cos(angles), jnp.sin(angles)
        cos_t = jnp.concatenate([cos_v, cos_v], axis=-1)
        sin_t = jnp.concatenate([-sin_v, sin_v], axis=-1)
        q_seg = jnp.broadcast_to(own_seg.reshape(chips, BATCHES, unit, 1), (chips, BATCHES, unit, HEAD_DIM))
        k_seg = segs.reshape(n_sp * chips // 2, 1, 2 * BATCHES * unit)
        o_seg = own_seg.reshape(chips, 1, BATCHES * unit)

        vmem = pl.BlockSpec(memory_space=pltpu.VMEM)
        hbm = pl.BlockSpec(memory_space=pl.ANY)
        dma = pltpu.SemaphoreType.DMA
        rows_q = heads * unit
        cache = jax.ShapeDtypeStruct((n_layers, chips, CORES, BATCHES, sub, HEAD_DIM), BF16)
        out, k_c, v_c = pl.pallas_call(
            make_kernel(n_layers, n_sp, n_tp, sub, model_dim, q_dim, ffn, col),
            name='decoder_stack',
            out_shape=(jax.ShapeDtypeStruct((BATCHES, sub, model_dim), BF16), cache, cache),
            in_specs=[vmem] * 8 + [hbm] * 7,
            out_specs=(vmem, hbm, hbm),
            scratch_shapes=[
                pltpu.VMEM((BATCHES, sub, model_dim), BF16),
                pltpu.VMEM((BATCHES, chips, CORES, sub, model_dim), BF16),
                pltpu.VMEM((4, CORES, sub, model_dim), BF16),
                pltpu.VMEM((BATCHES, 4, sub, model_dim), BF16),
                pltpu.VMEM((BATCHES, 2, sub // 2, model_dim), BF16),
                pltpu.VMEM((BATCHES, 2, sub, model_dim), BF16),
                pltpu.VMEM((BATCHES, 4, unit, ffn), BF16),
                pltpu.VMEM((BATCHES, 4, heads, unit, HEAD_DIM), BF16),
                pltpu.VMEM((BATCHES, 4, rows_q, HEAD_DIM), F32),
                pltpu.VMEM((BATCHES, 4, rows_q, HEAD_DIM), F32),
                pltpu.VMEM((BATCHES, 4, rows_q, HEAD_DIM), F32),
                pltpu.VMEM((n_layers, n_sp, chips, BATCHES, CORES, sub, 2 * HEAD_DIM), BF16),
                pltpu.VMEM((model_dim, q_dim + 2 * HEAD_DIM), BF16),
                pltpu.VMEM((q_dim, model_dim), BF16),
                pltpu.VMEM((model_dim, ffn), BF16),
                pltpu.VMEM((model_dim, ffn), BF16),
                pltpu.VMEM((ffn, model_dim), BF16),
                dma((7,)),
                dma((BATCHES, 10)), dma((BATCHES,)), dma((BATCHES, 2)), dma((BATCHES, 2)), dma((BATCHES, 2)), dma((BATCHES, 3)),
                dma((BATCHES, 4)), dma((BATCHES, 4)), dma((BATCHES, 6)), dma((BATCHES, 2)), dma((BATCHES, 2, 2)),
                dma((n_sp - 1,)), dma((n_layers, n_sp)), dma((BATCHES, CORES, 2)),
            ],
            compiler_params=pltpu.CompilerParams(collective_id=0, has_side_effects=True, vmem_limit_bytes=67_000_000),
        )(hidden_in.reshape(BATCHES, sub, model_dim), cos_t, sin_t, q_seg, k_seg, o_seg,
          attn_gain.astype(F32).reshape(n_layers, 1, model_dim), mlp_gain.astype(F32).reshape(n_layers, 1, model_dim),
          w_q, w_k, w_v, w_o, w_gate, w_up, w_down)
        cache_shape = (n_layers, n_rows, 1, HEAD_DIM)
        return out.reshape(tok_local, model_dim), k_c.reshape(cache_shape), v_c.reshape(cache_shape)

    return jax.shard_map(device_fn, mesh=mesh,
                         in_specs=(P(('dp', 'sp', 'tp'), None), tok_spec, tok_spec, P(), col_spec, col_spec, col_spec, row_spec, P(), col_spec, col_spec, row_spec),
                         out_specs=(P(('dp', 'sp', 'tp'), None), cache_spec, cache_spec), check_vma=False)
```

```python
import jax
import jax.numpy as jnp
from jax import lax
from jax.experimental import pallas as pl
from jax.experimental.pallas import tpu as pltpu
from jax.sharding import PartitionSpec as P

HEAD_DIM = 128
ROPE_BASE = 1e4
NORM_EPS = 1e-5
LOG2E = 1.4426950408889634
SCORE_EXP2 = HEAD_DIM ** -0.5 * LOG2E
NEG = -1e30
SPLIT = 2.0 ** 99
MESH = pl.DeviceIdType.MESH
F32 = jnp.float32
BF16 = jnp.bfloat16
CORES = 2
BATCHES = 2
OPP, RIGHT, LEFT, OWN = 0, 1, 2, 3


def dot(a, b):
    return jnp.dot(a, b, preferred_element_type=F32)


def make_kernel(n_layers, n_sp, n_tp, sub, model_dim, q_dim, ffn, col):
    chips = n_tp // CORES
    half = sub // 2
    unit = CORES * sub
    heads = q_dim // HEAD_DIM
    chip_rows = BATCHES * unit

    def kernel(hid, tab_own, hot_own, gain_a, gain_m, wq_h, wk_h, wv_h, wo_h, wg_h, wu_h, wd_h,
               out, k_out, v_out,
               res, gath, part, acc_rs, opp_in, nb_in, act, q_buf, m_buf, l_buf, o_buf, kv, tab, hot,
               w_qkv, w_o, w_g, w_u, w_d,
               w_sem, ag_send, ag_sib, ag_l, ag_r, ag_o, ag_sf, rs_dsend, rs_sib, rs_send, rs_opp, rs_nb, kv_send, kv_recv, c_sem, t_send, t_recv, h_send, h_recv, e_send, e_recv):
        y = lax.axis_index('sp')
        me = lax.axis_index('tp')
        x = me // CORES
        c = lax.rem(me, CORES)
        oc = 1 - c
        xl = lax.rem(x + chips - 1, chips)
        xr = lax.rem(x + 1, chips)
        xo = lax.rem(x + 2, chips)

        def unit_of(k):
            if isinstance(k, int):
                return (xo, xr, xl, x)[k]
            p, i = k // 2, lax.rem(k, 2)
            return lax.rem(x + (2 + p) * (1 - i) + (1 - p) * i, chips)
        sib = {'tp': x * CORES + oc}
        right = {'tp': xr * CORES + c}
        left = {'tp': xl * CORES + c}
        lo = pl.ds(0, half)
        hi = pl.ds(half, half)

        def rdma(src, dst, ssem, rsem, dev):
            return pltpu.make_async_remote_copy(src_ref=src, dst_ref=dst, send_sem=ssem, recv_sem=rsem,
                                                device_id=dev, device_id_type=MESH)

        def attn_weights(l):
            return [pltpu.make_async_copy(wq_h.at[l], w_qkv.at[:, pl.ds(0, q_dim)], w_sem.at[0]),
                    pltpu.make_async_copy(wk_h.at[l], w_qkv.at[:, pl.ds(q_dim, HEAD_DIM)], w_sem.at[1]),
                    pltpu.make_async_copy(wv_h.at[l], w_qkv.at[:, pl.ds(q_dim + HEAD_DIM, HEAD_DIM)], w_sem.at[2]),
                    pltpu.make_async_copy(wo_h.at[l], w_o, w_sem.at[3])]

        def mlp_weights(l):
            return [pltpu.make_async_copy(wg_h.at[l], w_g, w_sem.at[4]),
                    pltpu.make_async_copy(wu_h.at[l], w_u, w_sem.at[5]),
                    pltpu.make_async_copy(wd_h.at[l], w_d, w_sem.at[6])]

        for cp in attn_weights(0) + mlp_weights(0):
            cp.start()

        barrier = pltpu.get_barrier_semaphore()
        for t in range(1, n_tp):
            pl.semaphore_signal(barrier, inc=1, device_id={'tp': lax.rem(me + t, n_tp)}, device_id_type=MESH)
        for d in range(1, n_sp):
            pl.semaphore_signal(barrier, inc=1, device_id={'sp': lax.rem(y + d, n_sp)}, device_id_type=MESH)
        pl.semaphore_wait(barrier, n_tp - 1 + n_sp - 1)

        def ag_copies(b):
            own = gath.at[b, x, c]
            return {
                'sib': lambda: rdma(own, own, ag_send.at[b, 0], ag_sib.at[b], sib),
                'r_lo': lambda: rdma(own.at[lo], own.at[lo], ag_send.at[b, 1], ag_l.at[b, 0], right),
                'l_hi': lambda: rdma(own.at[hi], own.at[hi], ag_send.at[b, 2], ag_r.at[b, 1], left),
                'r_hi': lambda: rdma(own.at[hi], own.at[hi], ag_send.at[b, 3], ag_l.at[b, 1], right),
                'l_lo': lambda: rdma(own.at[lo], own.at[lo], ag_send.at[b, 4], ag_r.at[b, 0], left),
                'f_r': lambda: rdma(gath.at[b, xl, c, lo], gath.at[b, xl, c, lo], ag_send.at[b, 5], ag_o.at[b, 0], right),
                'f_l': lambda: rdma(gath.at[b, xr, c, hi], gath.at[b, xr, c, hi], ag_send.at[b, 6], ag_o.at[b, 1], left),
                's_l': lambda: rdma(gath.at[b, xl, c], gath.at[b, xl, c], ag_send.at[b, 7], ag_sf.at[b, LEFT], sib),
                's_r': lambda: rdma(gath.at[b, xr, c], gath.at[b, xr, c], ag_send.at[b, 8], ag_sf.at[b, RIGHT], sib),
                's_o': lambda: rdma(gath.at[b, xo, c], gath.at[b, xo, c], ag_send.at[b, 9], ag_sf.at[b, OPP], sib),
            }

        def arrived(ref, sem):
            rdma(ref, ref, ag_send.at[0, 0], sem, sib).wait_recv()

        def ag0a(b):
            cps = ag_copies(b)
            for name in ('sib', 'r_lo', 'l_hi'):
                cps[name]().start()

        def ag0b(b):
            cps = ag_copies(b)
            for name in ('r_hi', 'l_lo'):
                cps[name]().start()

        def ag1(b):
            cps = ag_copies(b)
            arrived(gath.at[b, xl, c, lo], ag_l.at[b, 0])
            cps['f_r']().start()
            arrived(gath.at[b, xr, c, hi], ag_r.at[b, 1])
            cps['f_l']().start()

        def ag2(b):
            cps = ag_copies(b)
            arrived(gath.at[b, xl, c, hi], ag_l.at[b, 1])
            cps['s_l']().start()
            arrived(gath.at[b, xr, c, lo], ag_r.at[b, 0])
            cps['s_r']().start()

        def ag3(b):
            cps = ag_copies(b)
            arrived(gath.at[b, xo, c, lo], ag_o.at[b, 0])
            arrived(gath.at[b, xo, c, hi], ag_o.at[b, 1])
            cps['s_o']().start()

        def ag_unit_ready(b, k):
            arrived(gath.at[b, unit_of(k), oc], ag_sib.at[b] if isinstance(k, int) and k == OWN else ag_sf.at[b, k])

        def ag_sent(b):
            for cp in ag_copies(b).values():
                cp().wait_send()

        def rs_pair(b, k):
            return rdma(part.at[k, oc], acc_rs.at[b, k], rs_dsend.at[b, k], rs_sib.at[b, k], sib)

        def rs_copies(b):
            return {
                'o_r': lambda: rdma(acc_rs.at[b, OPP, lo], opp_in.at[b, 0], rs_send.at[b, 0], rs_opp.at[b, 0], right),
                'o_l': lambda: rdma(acc_rs.at[b, OPP, hi], opp_in.at[b, 1], rs_send.at[b, 1], rs_opp.at[b, 1], left),
                'r_hi': lambda: rdma(acc_rs.at[b, RIGHT, hi], nb_in.at[b, 0, hi], rs_send.at[b, 2], rs_nb.at[b, 0, 1], right),
                'l_lo': lambda: rdma(acc_rs.at[b, LEFT, lo], nb_in.at[b, 1, lo], rs_send.at[b, 3], rs_nb.at[b, 1, 0], left),
                'r_lo': lambda: rdma(acc_rs.at[b, RIGHT, lo], nb_in.at[b, 0, lo], rs_send.at[b, 4], rs_nb.at[b, 0, 0], right),
                'l_hi': lambda: rdma(acc_rs.at[b, LEFT, hi], nb_in.at[b, 1, hi], rs_send.at[b, 5], rs_nb.at[b, 1, 1], left),
            }

        def pair_sum(b, k):
            cp = rs_pair(b, k)
            cp.wait_send()
            cp.wait_recv()
            acc_rs[b, k] = (acc_rs[b, k].astype(F32) + part[k, c].astype(F32)).astype(BF16)

        def rs1(b):
            pair_sum(b, OPP)
            cps = rs_copies(b)
            cps['o_r']().start()
            cps['o_l']().start()

        def rs2a(b):
            cps = rs_copies(b)
            pair_sum(b, RIGHT)
            cps['r_hi']().start()
            pair_sum(b, LEFT)
            cps['l_lo']().start()
            pair_sum(b, OWN)

        def rs2b(b):
            cps = rs_copies(b)
            cps['o_r']().wait_recv()
            acc_rs[b, RIGHT, lo] = (acc_rs[b, RIGHT, lo].astype(F32) + opp_in[b, 0].astype(F32)).astype(BF16)
            cps['r_lo']().start()
            cps['o_l']().wait_recv()
            acc_rs[b, LEFT, hi] = (acc_rs[b, LEFT, hi].astype(F32) + opp_in[b, 1].astype(F32)).astype(BF16)
            cps['l_hi']().start()

        def fin(b):
            cps = rs_copies(b)
            for name in ('r_hi', 'l_lo', 'r_lo', 'l_hi'):
                cps[name]().wait_recv()
            for cp in cps.values():
                cp().wait_send()
            total = (acc_rs[b, OWN].astype(F32) + nb_in[b, 0].astype(F32) + nb_in[b, 1].astype(F32)).astype(BF16)
            res[b] = (res[b].astype(F32) + total.astype(F32)).astype(BF16)

        def norm(b, gain):
            h = res[b].astype(F32)
            inv = lax.rsqrt(jnp.mean(h * h, axis=-1, keepdims=True) + NORM_EPS)
            gath[b, x, c] = (h * inv * gain).astype(BF16)

        def gain_row(ref, l):
            row = ref[0:1]
            for i in range(1, n_layers):
                row = jnp.where(l == i, ref[i:i + 1], row)
            return row

        def store_part(k, lhs, w, n):
            cols = pl.ds(n * col if isinstance(n, int) else pl.multiple_of(n * col, col), col)
            r = dot(lhs, w[:, cols]).astype(BF16)
            part[k, :, :, cols] = r.reshape(CORES, sub, col)

        def rope(v, cos_v, sin_v):
            return v * cos_v + pltpu.roll(v, HEAD_DIM // 2, 1) * sin_v

        def qkv(l, b, k):
            ag_unit_ready(b, k)
            u = unit_of(k)
            n = gath[b, u].reshape(unit, model_dim)
            packed = tab[b, u].reshape(unit, HEAD_DIM)
            swapped = pltpu.roll(packed, HEAD_DIM // 2, 1)
            first = lax.broadcasted_iota(jnp.int32, (unit, HEAD_DIM), 1) < HEAD_DIM // 2
            cos_v = jnp.where(first, packed, swapped)
            sin_v = jnp.where(first, -swapped, packed)
            away = ((hot[y, b, u].reshape(unit, HEAD_DIM).astype(F32) - 1.0) * SPLIT).astype(BF16)
            for h0 in range(0, heads + 2, 2):
                width = min(2, heads + 2 - h0) * HEAD_DIM
                r = dot(n, w_qkv[:, pl.ds(h0 * HEAD_DIM, width)])
                for h in range(h0, min(h0 + 2, heads + 2)):
                    v = r[:, (h - h0) * HEAD_DIM:(h - h0 + 1) * HEAD_DIM]
                    if h < heads:
                        q_buf[b, k, h, :, pl.ds(0, HEAD_DIM)] = rope(v, cos_v, sin_v).astype(BF16)
                        q_buf[b, k, h, :, pl.ds(HEAD_DIM, HEAD_DIM)] = away
                    elif h == heads:
                        kv[l, y, b, u, :, :, pl.ds(0, HEAD_DIM)] = rope(v, cos_v, sin_v).astype(BF16).reshape(CORES, sub, HEAD_DIM)
                    else:
                        kv[l, y, b, u, :, :, pl.ds(HEAD_DIM, HEAD_DIM)] = v.astype(BF16).reshape(CORES, sub, HEAD_DIM)
            m_buf[b, k] = jnp.full(m_buf.shape[2:], NEG, F32)
            l_buf[b, k] = jnp.zeros(l_buf.shape[2:], F32)
            o_buf[b, k] = jnp.zeros(o_buf.shape[2:], F32)
            for d in range(1, n_sp):
                @pl.when(y + d < n_sp)
                def _():
                    kv_copy(b, l, kv.at[l, y, b, u], d).start()

        def kv_copy(b, l, ref, d):
            return rdma(ref, ref, kv_send.at[b, d - 1], kv_recv.at[l, y, b], {'sp': lax.min(y + d, n_sp - 1)})

        def cache_copies(l):
            cps = []
            for b in range(BATCHES):
                for core in range(CORES):
                    for i, ref in enumerate((k_out, v_out)):
                        cps.append(pltpu.make_async_copy(kv.at[l, y, b, :, core, :, pl.ds(i * HEAD_DIM, HEAD_DIM)],
                                                         ref.at[l, :, core, b], c_sem.at[b, core, i]))
            return cps

        def flash(b, ks, block, marks, masks=None):
            n_keys = block.shape[0]
            keys = jnp.concatenate([block[:, :HEAD_DIM], marks], axis=1)
            vals = block[:, HEAD_DIM:]
            scores = [lax.dot_general(keys, q_buf[b, k].reshape(heads * unit, 2 * HEAD_DIM), (((1,), (1,)), ((), ())),
                                      preferred_element_type=F32) for k in ks]
            for i, k in enumerate(ks):
                s = scores[i]
                if masks is not None:
                    s = jnp.where(masks[i], s, NEG)
                m_old = m_buf[b, k]
                m_new = jnp.maximum(m_old, jnp.max(s, axis=0, keepdims=True))
                alpha = jnp.exp2((m_old - m_new) * SCORE_EXP2)
                p = jnp.exp2((s - m_new[0:1]) * SCORE_EXP2)
                m_buf[b, k] = m_new
                l_buf[b, k] = l_buf[b, k] * alpha + jnp.sum(p.reshape(n_keys // 8, 8, heads * unit), axis=0)
                o_buf[b, k] = o_buf[b, k] * alpha[0:1] + lax.dot_general(vals, p.astype(BF16), (((0,), (0,)), ((), ())),
                                                                         preferred_element_type=F32)

        def row_block(l, r, kb):
            return kv[l, r, kb].reshape(chips * unit, 2 * HEAD_DIM), hot[r, kb].reshape(chips * unit, HEAD_DIM)

        def attn_below(l, b, p, kb):
            def step(r, carry):
                flash(b, (2 * p, 2 * p + 1), *row_block(l, r, kb))
                return carry

            lax.fori_loop(0, y, step, 0)

        def kv_ready(l, kb):
            for r in range(n_sp - 1):
                @pl.when(r < y)
                def _():
                    rdma(kv.at[l, r, kb], kv.at[l, r, kb], kv_send.at[0, 0], kv_recv.at[l, r, kb], sib).wait_recv()

        def attn_own(l, b, p, kb):
            key = lax.broadcasted_iota(jnp.int32, (chips * unit, unit), 0)
            qry = lax.broadcasted_iota(jnp.int32, (chips * unit, unit), 1)
            ahead = (qry // sub - key // sub) * (BATCHES * sub) + lax.rem(qry, sub) - lax.rem(key, sub) + (b - kb) * sub
            ks = (2 * p, 2 * p + 1)
            masks = [jnp.concatenate([ahead >= -unit_of(k) * chip_rows] * heads, axis=1) for k in ks]
            flash(b, ks, *row_block(l, y, kb), masks)

        def attn_out(b, p):
            def one(i, carry):
                k = 2 * p + i
                o = o_buf[b, k] * (1.0 / jnp.sum(l_buf[b, k], axis=0, keepdims=True))
                o = jnp.concatenate([o[:, h * unit:(h + 1) * unit].T.astype(BF16) for h in range(heads)], axis=1)
                for n in range(model_dim // col):
                    store_part(k, o, w_o, n)
                rs_pair(b, k).start()
                return carry

            lax.fori_loop(0, 2, one, 0)

        ffn_col = min(1024, ffn)

        def gate_up(b, k):
            ag_unit_ready(b, k)
            n = gath[b, unit_of(k)].reshape(unit, model_dim)

            def step(j, carry):
                cols = pl.ds(j * ffn_col, ffn_col)
                g = dot(n, w_g[:, cols])
                act[b, k, :, cols] = (g * jax.nn.sigmoid(g) * dot(n, w_u[:, cols])).astype(BF16)
                return carry

            for j in range(ffn // ffn_col):
                step(j, 0)

        def down(b, p):
            def one(i, carry):
                k = 2 * p + i
                for n in range(model_dim // col):
                    store_part(k, act[b, k], w_d, n)
                rs_pair(b, k).start()
                return carry

            lax.fori_loop(0, 2, one, 0)

        def sides(fn, b):
            def one(i, carry):
                fn(b, LEFT - i)
                return carry

            lax.fori_loop(0, 2, one, 0)

        A, B = 0, 1
        res[...] = hid[...]
        norm(A, gain_row(gain_a, 0))
        ag0a(A)
        tab[:, x, c] = tab_own[...]
        hot[y, :, x, c] = hot_own[...]

        def peer_copies(t, src):
            to = {'tp': lax.rem(me + t, n_tp)}
            return (rdma(tab_own, tab.at[:, src // CORES, lax.rem(src, CORES)], t_send.at[t], t_recv.at[src], to),
                    rdma(hot_own, hot.at[y, :, src // CORES, lax.rem(src, CORES)], h_send.at[t], h_recv.at[src], to))

        def hot_copy(d):
            return rdma(hot.at[y], hot.at[y], e_send.at[d - 1], e_recv.at[y], {'sp': lax.min(y + d, n_sp - 1)})

        for t in range(1, n_tp):
            for cp in peer_copies(t, me):
                cp.start()
        for t in range(1, n_tp):
            for cp in peer_copies(t, lax.rem(me + t, n_tp)):
                cp.wait_recv()
        for d in range(1, n_sp):
            @pl.when(y + d < n_sp)
            def _():
                hot_copy(d).start()

        def layer(l, carry):
            more = l + 1 < n_layers
            nxt = lax.min(l + 1, n_layers - 1)
            for cp in attn_weights(l)[:3]:
                cp.wait()
            def qkv_l(b, k):
                qkv(l, b, k)

            qkv(l, A, OWN)

            @pl.when(l > 0)
            def _():
                rs2b(B)
            ag0b(A)
            ag1(A)

            @pl.when(l > 0)
            def _():
                fin(B)
            norm(B, gain_row(gain_a, l))
            ag0a(B)
            ag2(A)
            ag0b(B)
            sides(qkv_l, A)
            ag3(A)
            qkv(l, B, OWN)
            ag1(B)
            qkv(l, A, OPP)

            @pl.when(l == 0)
            def _():
                for r in range(n_sp - 1):
                    @pl.when(r < y)
                    def _():
                        rdma(hot.at[r], hot.at[r], e_send.at[0], e_recv.at[r], sib).wait_recv()
            kv_ready(l, A)

            def early(p, carry):
                attn_below(l, A, p, A)
                attn_own(l, A, p, A)
                return carry

            lax.fori_loop(0, 2, early, 0)
            ag2(B)
            sides(qkv_l, B)
            ag3(B)
            attn_weights(l)[3].wait()
            ag_sent(A)
            qkv(l, B, OPP)
            for cp in cache_copies(l):
                cp.start()

            def late_a(p, carry):
                attn_own(l, A, p, B)

                @pl.when(p == 0)
                def _():
                    kv_ready(l, B)
                attn_below(l, A, p, B)
                attn_out(A, p)

                @pl.when(p == 0)
                def _():
                    rs1(A)
                return carry

            lax.fori_loop(0, 2, late_a, 0)
            rs2a(A)
            ag_sent(B)

            def late_b(p, carry):
                def keys(kb, carry):
                    attn_below(l, B, p, kb)
                    attn_own(l, B, p, kb)
                    return carry

                lax.fori_loop(0, BATCHES, keys, 0)

                @pl.when(p == 0)
                def _():
                    rs2b(A)
                attn_out(B, p)

                @pl.when(p == 0)
                def _():
                    rs1(B)
                return carry

            lax.fori_loop(0, 2, late_b, 0)

            @pl.when(more)
            def _():
                for cp in attn_weights(nxt):
                    cp.start()
            fin(A)
            norm(A, gain_row(gain_m, l))
            rs2a(B)
            ag0a(A)
            for cp in mlp_weights(l)[:2]:
                cp.wait()
            gate_up(A, OWN)
            rs2b(B)
            ag0b(A)
            ag1(A)
            fin(B)
            norm(B, gain_row(gain_m, l))
            ag0a(B)
            ag2(A)
            ag0b(B)
            sides(gate_up, A)
            ag3(A)
            gate_up(B, OWN)
            ag1(B)
            gate_up(A, OPP)
            mlp_weights(l)[2].wait()
            ag_sent(A)
            down(A, 0)
            rs1(A)
            down(A, 1)
            ag2(B)
            gate_up(B, RIGHT)
            rs2a(A)
            ag3(B)
            gate_up(B, OPP)
            ag_sent(B)
            down(B, 0)
            rs2b(A)
            rs1(B)
            gate_up(B, LEFT)
            down(B, 1)

            @pl.when(more)
            def _():
                for cp in mlp_weights(nxt):
                    cp.start()
            rs2a(B)
            fin(A)

            @pl.when(more)
            def _():
                norm(A, gain_row(gain_a, nxt))
                ag0a(A)
            for cp in cache_copies(l):
                cp.wait()
            for d in range(1, n_sp):
                @pl.when(y + d < n_sp)
                def _():
                    for b in range(BATCHES):
                        kv_copy(b, l, kv.at[l, y, b], d).wait_send()
            return carry

        lax.fori_loop(0, n_layers, layer, 0)
        rs2b(B)
        fin(B)
        out[...] = res[...]
        for t in range(1, n_tp):
            for cp in peer_copies(t, me):
                cp.wait_send()
        for d in range(1, n_sp):
            @pl.when(y + d < n_sp)
            def _():
                hot_copy(d).wait_send()

    return kernel


def solution(mesh):
    n_sp, n_tp = mesh.shape['sp'], mesh.shape['tp']
    chips = n_tp // CORES
    tok_spec = P(('dp', 'sp', 'tp'))
    col_spec = P(None, None, 'tp')
    row_spec = P(None, 'tp', None)
    cache_spec = P(None, ('dp', 'sp'), 'tp', None)

    def device_fn(hidden_in, segment_ids, positions, attn_gain, w_q, w_k, w_v, w_o, mlp_gain, w_gate, w_up, w_down):
        tok_local, model_dim = hidden_in.shape
        n_layers, _, q_dim = w_q.shape
        ffn = w_gate.shape[2]
        sub = tok_local // BATCHES
        unit = CORES * sub
        n_rows = tok_local * n_tp
        heads = q_dim // HEAD_DIM
        col = min(1536, model_dim)

        half_dim = HEAD_DIM // 2
        inv_freq = ROPE_BASE ** (-jnp.arange(half_dim, dtype=F32) / half_dim)
        angles = positions.reshape(BATCHES, sub, 1).astype(F32) * inv_freq
        tab = jnp.concatenate([jnp.cos(angles), jnp.sin(angles)], axis=-1)
        hot = (segment_ids.reshape(BATCHES, sub, 1) == jnp.arange(HEAD_DIM)).astype(BF16)

        vmem = pl.BlockSpec(memory_space=pltpu.VMEM)
        hbm = pl.BlockSpec(memory_space=pl.ANY)
        dma = pltpu.SemaphoreType.DMA
        rows_q = heads * unit
        cache = jax.ShapeDtypeStruct((n_layers, chips, CORES, BATCHES, sub, HEAD_DIM), BF16)
        out, k_c, v_c = pl.pallas_call(
            make_kernel(n_layers, n_sp, n_tp, sub, model_dim, q_dim, ffn, col),
            name='decoder_stack',
            out_shape=(jax.ShapeDtypeStruct((BATCHES, sub, model_dim), BF16), cache, cache),
            in_specs=[vmem] * 5 + [hbm] * 7,
            out_specs=(vmem, hbm, hbm),
            scratch_shapes=[
                pltpu.VMEM((BATCHES, sub, model_dim), BF16),
                pltpu.VMEM((BATCHES, chips, CORES, sub, model_dim), BF16),
                pltpu.VMEM((4, CORES, sub, model_dim), BF16),
                pltpu.VMEM((BATCHES, 4, sub, model_dim), BF16),
                pltpu.VMEM((BATCHES, 2, sub // 2, model_dim), BF16),
                pltpu.VMEM((BATCHES, 2, sub, model_dim), BF16),
                pltpu.VMEM((BATCHES, 4, unit, ffn), BF16),
                pltpu.VMEM((BATCHES, 4, heads, unit, 2 * HEAD_DIM), BF16),
                pltpu.VMEM((BATCHES, 4, 8, rows_q), F32),
                pltpu.VMEM((BATCHES, 4, 8, rows_q), F32),
                pltpu.VMEM((BATCHES, 4, HEAD_DIM, rows_q), F32),
                pltpu.VMEM((n_layers, n_sp, BATCHES, chips, CORES, sub, 2 * HEAD_DIM), BF16),
                pltpu.VMEM((BATCHES, chips, CORES, sub, HEAD_DIM), F32),
                pltpu.VMEM((n_sp, BATCHES, chips, CORES, sub, HEAD_DIM), BF16),
                pltpu.VMEM((model_dim, q_dim + 2 * HEAD_DIM), BF16),
                pltpu.VMEM((q_dim, model_dim), BF16),
                pltpu.VMEM((model_dim, ffn), BF16),
                pltpu.VMEM((model_dim, ffn), BF16),
                pltpu.VMEM((ffn, model_dim), BF16),
                dma((7,)),
                dma((BATCHES, 10)), dma((BATCHES,)), dma((BATCHES, 2)), dma((BATCHES, 2)), dma((BATCHES, 2)), dma((BATCHES, 3)),
                dma((BATCHES, 4)), dma((BATCHES, 4)), dma((BATCHES, 6)), dma((BATCHES, 2)), dma((BATCHES, 2, 2)),
                dma((BATCHES, n_sp - 1)), dma((n_layers, n_sp, BATCHES)), dma((BATCHES, CORES, 2)),
                dma((n_tp,)), dma((n_tp,)), dma((n_tp,)), dma((n_tp,)), dma((n_sp - 1,)), dma((n_sp,)),
            ],
            compiler_params=pltpu.CompilerParams(collective_id=0, has_side_effects=True, vmem_limit_bytes=67_000_000),
        )(hidden_in.reshape(BATCHES, sub, model_dim), tab, hot, attn_gain.astype(F32), mlp_gain.astype(F32),
          w_q, w_k, w_v, w_o, w_gate, w_up, w_down)
        cache_shape = (n_layers, n_rows, 1, HEAD_DIM)
        return out.reshape(tok_local, model_dim), k_c.reshape(cache_shape), v_c.reshape(cache_shape)

    return jax.shard_map(device_fn, mesh=mesh,
                         in_specs=(P(('dp', 'sp', 'tp'), None), tok_spec, tok_spec, P(), col_spec, col_spec, col_spec, row_spec, P(), col_spec, col_spec, row_spec),
                         out_specs=(P(('dp', 'sp', 'tp'), None), cache_spec, cache_spec), check_vma=False)
```

```python
import jax
import jax.numpy as jnp
from jax import lax
from jax.experimental import pallas as pl
from jax.experimental.pallas import tpu as pltpu
from jax.sharding import PartitionSpec as P

HEAD_DIM = 128
ROPE_BASE = 1e4
NORM_EPS = 1e-5
LOG2E = 1.4426950408889634
SCORE_EXP2 = HEAD_DIM ** -0.5 * LOG2E
NEG = -1e30
SPLIT = 2.0 ** 99
MESH = pl.DeviceIdType.MESH
F32 = jnp.float32
BF16 = jnp.bfloat16
CORES = 2
BATCHES = 2
OPP, RIGHT, LEFT, OWN = 0, 1, 2, 3


def dot(a, b):
    return jnp.dot(a, b, preferred_element_type=F32)


def make_kernel(n_layers, n_sp, n_tp, sub, model_dim, q_dim, ffn, col):
    chips = n_tp // CORES
    half = sub // 2
    unit = CORES * sub
    heads = q_dim // HEAD_DIM
    chip_rows = BATCHES * unit

    def kernel(hid, tab_own, hot_own, gain_a, gain_m, wq_h, wk_h, wv_h, wo_h, wg_h, wu_h, wd_h,
               out, k_out, v_out,
               res, gath, part, acc_rs, opp_in, nb_in, act, q_buf, m_buf, l_buf, o_buf, kv, tab, hot,
               w_qkv, w_o, w_g, w_u, w_d,
               w_sem, ag_send, ag_sib, ag_l, ag_r, ag_o, ag_sf, rs_dsend, rs_sib, rs_send, rs_opp, rs_nb, kv_send, kv_recv, c_sem, t_send, t_recv, h_send, h_recv, e_send, e_recv):
        y = lax.axis_index('sp')
        me = lax.axis_index('tp')
        x = me // CORES
        c = lax.rem(me, CORES)
        oc = 1 - c
        xl = lax.rem(x + chips - 1, chips)
        xr = lax.rem(x + 1, chips)
        xo = lax.rem(x + 2, chips)

        def unit_of(k):
            if isinstance(k, int):
                return (xo, xr, xl, x)[k]
            p, i = k // 2, lax.rem(k, 2)
            return lax.rem(x + (2 + p) * (1 - i) + (1 - p) * i, chips)
        sib = {'tp': x * CORES + oc}
        right = {'tp': xr * CORES + c}
        left = {'tp': xl * CORES + c}
        lo = pl.ds(0, half)
        hi = pl.ds(half, half)

        def rdma(src, dst, ssem, rsem, dev):
            return pltpu.make_async_remote_copy(src_ref=src, dst_ref=dst, send_sem=ssem, recv_sem=rsem,
                                                device_id=dev, device_id_type=MESH)

        def attn_weights(l):
            return [pltpu.make_async_copy(wq_h.at[l], w_qkv.at[:, pl.ds(0, q_dim)], w_sem.at[0]),
                    pltpu.make_async_copy(wk_h.at[l], w_qkv.at[:, pl.ds(q_dim, HEAD_DIM)], w_sem.at[1]),
                    pltpu.make_async_copy(wv_h.at[l], w_qkv.at[:, pl.ds(q_dim + HEAD_DIM, HEAD_DIM)], w_sem.at[2]),
                    pltpu.make_async_copy(wo_h.at[l], w_o, w_sem.at[3])]

        def mlp_weights(l):
            return [pltpu.make_async_copy(wg_h.at[l], w_g, w_sem.at[4]),
                    pltpu.make_async_copy(wu_h.at[l], w_u, w_sem.at[5]),
                    pltpu.make_async_copy(wd_h.at[l], w_d, w_sem.at[6])]

        for cp in attn_weights(0) + mlp_weights(0):
            cp.start()

        barrier = pltpu.get_barrier_semaphore()
        for t in range(1, n_tp):
            pl.semaphore_signal(barrier, inc=1, device_id={'tp': lax.rem(me + t, n_tp)}, device_id_type=MESH)
        for d in range(1, n_sp):
            pl.semaphore_signal(barrier, inc=1, device_id={'sp': lax.rem(y + d, n_sp)}, device_id_type=MESH)
        pl.semaphore_wait(barrier, n_tp - 1 + n_sp - 1)

        def ag_copies(b):
            own = gath.at[b, x, c]
            return {
                'sib': lambda: rdma(own, own, ag_send.at[b, 0], ag_sib.at[b], sib),
                'r_lo': lambda: rdma(own.at[lo], own.at[lo], ag_send.at[b, 1], ag_l.at[b, 0], right),
                'l_hi': lambda: rdma(own.at[hi], own.at[hi], ag_send.at[b, 2], ag_r.at[b, 1], left),
                'r_hi': lambda: rdma(own.at[hi], own.at[hi], ag_send.at[b, 3], ag_l.at[b, 1], right),
                'l_lo': lambda: rdma(own.at[lo], own.at[lo], ag_send.at[b, 4], ag_r.at[b, 0], left),
                'f_r': lambda: rdma(gath.at[b, xl, c, lo], gath.at[b, xl, c, lo], ag_send.at[b, 5], ag_o.at[b, 0], right),
                'f_l': lambda: rdma(gath.at[b, xr, c, hi], gath.at[b, xr, c, hi], ag_send.at[b, 6], ag_o.at[b, 1], left),
                's_l': lambda: rdma(gath.at[b, xl, c], gath.at[b, xl, c], ag_send.at[b, 7], ag_sf.at[b, LEFT], sib),
                's_r': lambda: rdma(gath.at[b, xr, c], gath.at[b, xr, c], ag_send.at[b, 8], ag_sf.at[b, RIGHT], sib),
                's_o': lambda: rdma(gath.at[b, xo, c], gath.at[b, xo, c], ag_send.at[b, 9], ag_sf.at[b, OPP], sib),
            }

        def arrived(ref, sem):
            rdma(ref, ref, ag_send.at[0, 0], sem, sib).wait_recv()

        def ag0a(b):
            cps = ag_copies(b)
            for name in ('sib', 'r_lo', 'l_hi'):
                cps[name]().start()

        def ag0b(b):
            cps = ag_copies(b)
            for name in ('r_hi', 'l_lo'):
                cps[name]().start()

        def ag1(b):
            cps = ag_copies(b)
            arrived(gath.at[b, xl, c, lo], ag_l.at[b, 0])
            cps['f_r']().start()
            arrived(gath.at[b, xr, c, hi], ag_r.at[b, 1])
            cps['f_l']().start()

        def ag2(b):
            cps = ag_copies(b)
            arrived(gath.at[b, xl, c, hi], ag_l.at[b, 1])
            cps['s_l']().start()
            arrived(gath.at[b, xr, c, lo], ag_r.at[b, 0])
            cps['s_r']().start()

        def ag3(b):
            cps = ag_copies(b)
            arrived(gath.at[b, xo, c, lo], ag_o.at[b, 0])
            arrived(gath.at[b, xo, c, hi], ag_o.at[b, 1])
            cps['s_o']().start()

        def ag_unit_ready(b, k):
            arrived(gath.at[b, unit_of(k), oc], ag_sib.at[b] if isinstance(k, int) and k == OWN else ag_sf.at[b, k])

        def ag_sent(b):
            for cp in ag_copies(b).values():
                cp().wait_send()

        def rs_pair(b, k):
            return rdma(part.at[k, oc], acc_rs.at[b, k], rs_dsend.at[b, k], rs_sib.at[b, k], sib)

        def rs_copies(b):
            return {
                'o_r': lambda: rdma(acc_rs.at[b, OPP, lo], opp_in.at[b, 0], rs_send.at[b, 0], rs_opp.at[b, 0], right),
                'o_l': lambda: rdma(acc_rs.at[b, OPP, hi], opp_in.at[b, 1], rs_send.at[b, 1], rs_opp.at[b, 1], left),
                'r_hi': lambda: rdma(acc_rs.at[b, RIGHT, hi], nb_in.at[b, 0, hi], rs_send.at[b, 2], rs_nb.at[b, 0, 1], right),
                'l_lo': lambda: rdma(acc_rs.at[b, LEFT, lo], nb_in.at[b, 1, lo], rs_send.at[b, 3], rs_nb.at[b, 1, 0], left),
                'r_lo': lambda: rdma(acc_rs.at[b, RIGHT, lo], nb_in.at[b, 0, lo], rs_send.at[b, 4], rs_nb.at[b, 0, 0], right),
                'l_hi': lambda: rdma(acc_rs.at[b, LEFT, hi], nb_in.at[b, 1, hi], rs_send.at[b, 5], rs_nb.at[b, 1, 1], left),
            }

        def pair_sum(b, k):
            cp = rs_pair(b, k)
            cp.wait_send()
            cp.wait_recv()
            acc_rs[b, k] = (acc_rs[b, k].astype(F32) + part[k, c].astype(F32)).astype(BF16)

        def rs1(b):
            pair_sum(b, OPP)
            cps = rs_copies(b)
            cps['o_r']().start()
            cps['o_l']().start()

        def rs2a(b):
            cps = rs_copies(b)
            pair_sum(b, RIGHT)
            cps['r_hi']().start()
            pair_sum(b, LEFT)
            cps['l_lo']().start()
            pair_sum(b, OWN)

        def rs2b(b):
            cps = rs_copies(b)
            cps['o_r']().wait_recv()
            acc_rs[b, RIGHT, lo] = (acc_rs[b, RIGHT, lo].astype(F32) + opp_in[b, 0].astype(F32)).astype(BF16)
            cps['r_lo']().start()
            cps['o_l']().wait_recv()
            acc_rs[b, LEFT, hi] = (acc_rs[b, LEFT, hi].astype(F32) + opp_in[b, 1].astype(F32)).astype(BF16)
            cps['l_hi']().start()

        def fin(b):
            cps = rs_copies(b)
            for name in ('r_hi', 'l_lo', 'r_lo', 'l_hi'):
                cps[name]().wait_recv()
            for cp in cps.values():
                cp().wait_send()
            total = (acc_rs[b, OWN].astype(F32) + nb_in[b, 0].astype(F32) + nb_in[b, 1].astype(F32)).astype(BF16)
            res[b] = (res[b].astype(F32) + total.astype(F32)).astype(BF16)

        def norm(b, gain):
            h = res[b].astype(F32)
            inv = lax.rsqrt(jnp.mean(h * h, axis=-1, keepdims=True) + NORM_EPS)
            gath[b, x, c] = (h * inv * gain).astype(BF16)

        def gain_row(ref, l):
            rows = ref[...].astype(F32)
            row = rows[0:1]
            for i in range(1, n_layers):
                row = jnp.where(l == i, rows[i:i + 1], row)
            return row

        def store_part(k, lhs, w, n):
            cols = pl.ds(n * col if isinstance(n, int) else pl.multiple_of(n * col, col), col)
            r = dot(lhs, w[:, cols]).astype(BF16)
            part[k, :, :, cols] = r.reshape(CORES, sub, col)

        def rope(v, cos_v, sin_v):
            return v * cos_v + pltpu.roll(v, HEAD_DIM // 2, 1) * sin_v

        def qkv(l, b, k):
            ag_unit_ready(b, k)
            u = unit_of(k)
            n = gath[b, u].reshape(unit, model_dim)
            packed = tab[b, u].reshape(unit, HEAD_DIM)
            swapped = pltpu.roll(packed, HEAD_DIM // 2, 1)
            first = lax.broadcasted_iota(jnp.int32, (unit, HEAD_DIM), 1) < HEAD_DIM // 2
            cos_v = jnp.where(first, packed, swapped)
            sin_v = jnp.where(first, -swapped, packed)
            away = ((hot[y, b, u].reshape(unit, HEAD_DIM).astype(F32) - 1.0) * SPLIT).astype(BF16)
            for h0 in range(0, heads + 2, 2):
                width = min(2, heads + 2 - h0) * HEAD_DIM
                r = dot(n, w_qkv[:, pl.ds(h0 * HEAD_DIM, width)])
                for h in range(h0, min(h0 + 2, heads + 2)):
                    v = r[:, (h - h0) * HEAD_DIM:(h - h0 + 1) * HEAD_DIM]
                    if h < heads:
                        q_buf[b, k, h, :, pl.ds(0, HEAD_DIM)] = rope(v, cos_v, sin_v).astype(BF16)
                        q_buf[b, k, h, :, pl.ds(HEAD_DIM, HEAD_DIM)] = away
                    elif h == heads:
                        kv[l, y, b, u, :, :, pl.ds(0, HEAD_DIM)] = rope(v, cos_v, sin_v).astype(BF16).reshape(CORES, sub, HEAD_DIM)
                    else:
                        kv[l, y, b, u, :, :, pl.ds(HEAD_DIM, HEAD_DIM)] = v.astype(BF16).reshape(CORES, sub, HEAD_DIM)
            m_buf[b, k] = jnp.full(m_buf.shape[2:], NEG, F32)
            l_buf[b, k] = jnp.zeros(l_buf.shape[2:], F32)
            o_buf[b, k] = jnp.zeros(o_buf.shape[2:], F32)
            for d in range(1, n_sp):
                @pl.when(y + d < n_sp)
                def _():
                    kv_copy(b, l, kv.at[l, y, b, u], d).start()

        def kv_copy(b, l, ref, d):
            return rdma(ref, ref, kv_send.at[b, d - 1], kv_recv.at[l, y, b], {'sp': lax.min(y + d, n_sp - 1)})

        def cache_copies(l):
            cps = []
            for b in range(BATCHES):
                for core in range(CORES):
                    for i, ref in enumerate((k_out, v_out)):
                        cps.append(pltpu.make_async_copy(kv.at[l, y, b, :, core, :, pl.ds(i * HEAD_DIM, HEAD_DIM)],
                                                         ref.at[l, :, core, b], c_sem.at[b, core, i]))
            return cps

        def flash(b, ks, block, marks, masks=None):
            n_keys = block.shape[0]
            keys = jnp.concatenate([block[:, :HEAD_DIM], marks], axis=1)
            vals = block[:, HEAD_DIM:]
            scores = [lax.dot_general(keys, q_buf[b, k].reshape(heads * unit, 2 * HEAD_DIM), (((1,), (1,)), ((), ())),
                                      preferred_element_type=F32) for k in ks]
            for i, k in enumerate(ks):
                s = scores[i]
                if masks is not None:
                    s = jnp.where(masks[i], s, NEG)
                m_old = m_buf[b, k]
                m_new = jnp.maximum(m_old, jnp.max(s, axis=0, keepdims=True))
                alpha = jnp.exp2((m_old - m_new) * SCORE_EXP2)
                p = jnp.exp2((s - m_new[0:1]) * SCORE_EXP2)
                m_buf[b, k] = m_new
                l_buf[b, k] = l_buf[b, k] * alpha + jnp.sum(p.reshape(n_keys // 8, 8, heads * unit), axis=0)
                o_buf[b, k] = o_buf[b, k] * alpha[0:1] + lax.dot_general(vals, p.astype(BF16), (((0,), (0,)), ((), ())),
                                                                         preferred_element_type=F32)

        def row_block(l, r, kb):
            return kv[l, r, kb].reshape(chips * unit, 2 * HEAD_DIM), hot[r, kb].reshape(chips * unit, HEAD_DIM)

        def whole_row(l, r):
            n = BATCHES * chips * unit
            return kv[l, r].reshape(n, 2 * HEAD_DIM), hot[r].reshape(n, HEAD_DIM)

        def attn_below(l, b, ks, a0, a1, b0, b1):
            n_a = a1 - a0

            def step(n, carry):
                kb = jnp.where(n >= n_a, 1, 0)
                flash(b, ks, *row_block(l, n + a0 + kb * (b0 - n_a - a0), kb))
                return carry

            lax.fori_loop(0, n_a + b1 - b0, step, 0)

        def attn_below_rows(l, b, ks):
            def step(r, carry):
                flash(b, ks, *whole_row(l, r))
                return carry

            lax.fori_loop(0, y, step, 0)

        def kv_ready(l, kb, first, last):
            for r in range(n_sp - 1):
                @pl.when(jnp.logical_and(r >= first, r < last))
                def _():
                    rdma(kv.at[l, r, kb], kv.at[l, r, kb], kv_send.at[0, 0], kv_recv.at[l, r, kb], sib).wait_recv()

        def attn_own(l, b, ks, kb=None):
            n_keys = chips * unit * (BATCHES if kb is None else 1)
            key = lax.broadcasted_iota(jnp.int32, (n_keys, unit), 0)
            qry = lax.broadcasted_iota(jnp.int32, (n_keys, unit), 1)
            k_batch = key // (chips * unit) if kb is None else kb
            k_tok = lax.rem(key, chips * unit) // sub * (BATCHES * sub) + lax.rem(key, sub) + k_batch * sub
            ahead = qry // sub * (BATCHES * sub) + lax.rem(qry, sub) + b * sub - k_tok
            masks = [jnp.concatenate([ahead >= -unit_of(k) * chip_rows] * heads, axis=1) for k in ks]
            flash(b, ks, *(whole_row(l, y) if kb is None else row_block(l, y, kb)), masks)

        def attn_out(b, p):
            def one(i, carry):
                k = 2 * p + i
                o = o_buf[b, k] * (1.0 / jnp.sum(l_buf[b, k], axis=0, keepdims=True))
                o = jnp.concatenate([o[:, h * unit:(h + 1) * unit].T.astype(BF16) for h in range(heads)], axis=1)
                for n in range(model_dim // col):
                    store_part(k, o, w_o, n)
                rs_pair(b, k).start()
                return carry

            lax.fori_loop(0, 2, one, 0)

        ffn_col = min(1024, ffn)

        def gate_up(b, k):
            ag_unit_ready(b, k)
            n = gath[b, unit_of(k)].reshape(unit, model_dim)

            def step(j, carry):
                cols = pl.ds(j * ffn_col, ffn_col)
                g = dot(n, w_g[:, cols])
                act[b, k, :, cols] = (g * jax.nn.sigmoid(g) * dot(n, w_u[:, cols])).astype(BF16)
                return carry

            for j in range(ffn // ffn_col):
                step(j, 0)

        def down(b, p):
            def one(i, carry):
                k = 2 * p + i
                for n in range(model_dim // col):
                    store_part(k, act[b, k], w_d, n)
                rs_pair(b, k).start()
                return carry

            lax.fori_loop(0, 2, one, 0)

        def sides(fn, b):
            def one(i, carry):
                fn(b, LEFT - i)
                return carry

            lax.fori_loop(0, 2, one, 0)

        A, B = 0, 1
        res[...] = hid[...]
        norm(A, gain_row(gain_a, 0))
        ag0a(A)
        tab[:, x, c] = tab_own[...]
        hot[y, :, x, c] = hot_own[...]

        def peer_copies(t, src):
            to = {'tp': lax.rem(me + t, n_tp)}
            return (rdma(tab_own, tab.at[:, src // CORES, lax.rem(src, CORES)], t_send.at[t], t_recv.at[src], to),
                    rdma(hot_own, hot.at[y, :, src // CORES, lax.rem(src, CORES)], h_send.at[t], h_recv.at[src], to))

        def hot_copy(d):
            return rdma(hot.at[y], hot.at[y], e_send.at[d - 1], e_recv.at[y], {'sp': lax.min(y + d, n_sp - 1)})

        for t in range(1, n_tp):
            for cp in peer_copies(t, me):
                cp.start()
        for t in range(1, n_tp):
            for cp in peer_copies(t, lax.rem(me + t, n_tp)):
                cp.wait_recv()
        for d in range(1, n_sp):
            @pl.when(y + d < n_sp)
            def _():
                hot_copy(d).start()

        def layer(l, carry):
            more = l + 1 < n_layers
            nxt = lax.min(l + 1, n_layers - 1)
            for cp in attn_weights(l)[:3]:
                cp.wait()
            def qkv_l(b, k):
                qkv(l, b, k)

            qkv(l, A, OWN)

            @pl.when(l > 0)
            def _():
                rs2b(B)
            ag0b(A)
            ag1(A)

            @pl.when(l > 0)
            def _():
                fin(B)
            norm(B, gain_row(gain_a, l))
            ag0a(B)
            ag2(A)
            ag0b(B)
            sides(qkv_l, A)
            ahead = lax.max(y - 1, 0)
            a_soon = jnp.where(l > 0, ahead, 0)
            b_soon = jnp.where(l > 1, ahead, 0)
            b_early = jnp.where(l > 0, ahead, 0)

            def early(e, carry):
                @pl.when(e == 1)
                def _():
                    ag3(A)
                    qkv(l, B, OWN)
                    ag1(B)
                    qkv(l, A, OPP)

                    @pl.when(l == 0)
                    def _():
                        for r in range(n_sp - 1):
                            @pl.when(r < y)
                            def _():
                                rdma(hot.at[r], hot.at[r], e_send.at[0], e_recv.at[r], sib).wait_recv()

                a0, a1 = jnp.where(e == 0, 0, a_soon), jnp.where(e == 0, a_soon, y)
                b0, b1 = jnp.where(e == 0, 0, b_soon), jnp.where(e == 0, b_soon, b_early)
                kv_ready(l, A, a0, a1)
                kv_ready(l, B, b0, b1)
                attn_below(l, A, (RIGHT, LEFT, OWN), a0, a1, b0, b1)
                return carry

            lax.fori_loop(0, 2, early, 0)
            attn_below(l, A, (OPP,), 0, y, 0, b_early)
            attn_own(l, A, (OPP, RIGHT, LEFT, OWN), A)
            ag2(B)
            sides(qkv_l, B)
            ag3(B)
            attn_weights(l)[3].wait()
            ag_sent(A)
            qkv(l, B, OPP)
            for cp in cache_copies(l):
                cp.start()

            def late_a(p, carry):
                ks = (2 * p, 2 * p + 1)
                attn_own(l, A, ks, B)

                @pl.when(p == 0)
                def _():
                    kv_ready(l, B, b_early, y)
                attn_below(l, A, ks, 0, 0, b_early, y)
                attn_out(A, p)

                @pl.when(p == 0)
                def _():
                    rs1(A)
                return carry

            lax.fori_loop(0, 2, late_a, 0)
            rs2a(A)
            ag_sent(B)

            def late_b(p, carry):
                ks = (2 * p, 2 * p + 1)
                attn_own(l, B, ks)

                @pl.when(p == 0)
                def _():
                    rs2b(A)
                attn_below_rows(l, B, ks)
                attn_out(B, p)

                @pl.when(p == 0)
                def _():
                    rs1(B)
                    fin(A)
                    norm(A, gain_row(gain_m, l))
                    ag0a(A)
                return carry

            lax.fori_loop(0, 2, late_b, 0)

            @pl.when(more)
            def _():
                for cp in attn_weights(nxt):
                    cp.start()
            rs2a(B)
            for cp in mlp_weights(l)[:2]:
                cp.wait()
            gate_up(A, OWN)
            rs2b(B)
            ag0b(A)
            ag1(A)
            fin(B)
            norm(B, gain_row(gain_m, l))
            ag0a(B)
            ag2(A)
            ag0b(B)
            sides(gate_up, A)
            ag3(A)
            gate_up(B, OWN)
            ag1(B)
            gate_up(A, OPP)
            mlp_weights(l)[2].wait()
            ag_sent(A)
            down(A, 0)
            rs1(A)
            down(A, 1)
            ag2(B)

            def two(i, carry):
                gate_up(B, RIGHT - i)

                @pl.when(i == 0)
                def _():
                    rs2a(A)
                    ag3(B)
                return carry

            lax.fori_loop(0, 2, two, 0)
            ag_sent(B)
            down(B, 0)
            rs2b(A)
            rs1(B)
            gate_up(B, LEFT)
            down(B, 1)

            @pl.when(more)
            def _():
                for cp in mlp_weights(nxt):
                    cp.start()
            rs2a(B)
            fin(A)

            @pl.when(more)
            def _():
                norm(A, gain_row(gain_a, nxt))
                ag0a(A)
            for cp in cache_copies(l):
                cp.wait()
            for d in range(1, n_sp):
                @pl.when(y + d < n_sp)
                def _():
                    for b in range(BATCHES):
                        kv_copy(b, l, kv.at[l, y, b], d).wait_send()
            return carry

        lax.fori_loop(0, n_layers, layer, 0)
        rs2b(B)
        fin(B)
        out[...] = res[...]
        for t in range(1, n_tp):
            for cp in peer_copies(t, me):
                cp.wait_send()
        for d in range(1, n_sp):
            @pl.when(y + d < n_sp)
            def _():
                hot_copy(d).wait_send()

    return kernel


def solution(mesh):
    n_sp, n_tp = mesh.shape['sp'], mesh.shape['tp']
    chips = n_tp // CORES
    tok_spec = P(('dp', 'sp', 'tp'))
    col_spec = P(None, None, 'tp')
    row_spec = P(None, 'tp', None)
    cache_spec = P(None, ('dp', 'sp'), 'tp', None)

    def device_fn(hidden_in, segment_ids, positions, attn_gain, w_q, w_k, w_v, w_o, mlp_gain, w_gate, w_up, w_down):
        tok_local, model_dim = hidden_in.shape
        n_layers, _, q_dim = w_q.shape
        ffn = w_gate.shape[2]
        sub = tok_local // BATCHES
        unit = CORES * sub
        n_rows = tok_local * n_tp
        heads = q_dim // HEAD_DIM
        col = min(1536, model_dim)

        half_dim = HEAD_DIM // 2
        inv_freq = ROPE_BASE ** (-jnp.arange(half_dim, dtype=F32) / half_dim)
        angles = positions.reshape(BATCHES, sub, 1).astype(F32) * inv_freq
        tab = jnp.concatenate([jnp.cos(angles), jnp.sin(angles)], axis=-1)
        hot = (segment_ids.reshape(BATCHES, sub, 1) == jnp.arange(HEAD_DIM)).astype(BF16)

        vmem = pl.BlockSpec(memory_space=pltpu.VMEM)
        hbm = pl.BlockSpec(memory_space=pl.ANY)
        dma = pltpu.SemaphoreType.DMA
        rows_q = heads * unit
        cache = jax.ShapeDtypeStruct((n_layers, chips, CORES, BATCHES, sub, HEAD_DIM), BF16)
        out, k_c, v_c = pl.pallas_call(
            make_kernel(n_layers, n_sp, n_tp, sub, model_dim, q_dim, ffn, col),
            name='decoder_stack',
            out_shape=(jax.ShapeDtypeStruct((BATCHES, sub, model_dim), BF16), cache, cache),
            in_specs=[vmem] * 5 + [hbm] * 7,
            out_specs=(vmem, hbm, hbm),
            scratch_shapes=[
                pltpu.VMEM((BATCHES, sub, model_dim), BF16),
                pltpu.VMEM((BATCHES, chips, CORES, sub, model_dim), BF16),
                pltpu.VMEM((4, CORES, sub, model_dim), BF16),
                pltpu.VMEM((BATCHES, 4, sub, model_dim), BF16),
                pltpu.VMEM((BATCHES, 2, sub // 2, model_dim), BF16),
                pltpu.VMEM((BATCHES, 2, sub, model_dim), BF16),
                pltpu.VMEM((BATCHES, 4, unit, ffn), BF16),
                pltpu.VMEM((BATCHES, 4, heads, unit, 2 * HEAD_DIM), BF16),
                pltpu.VMEM((BATCHES, 4, 8, rows_q), F32),
                pltpu.VMEM((BATCHES, 4, 8, rows_q), F32),
                pltpu.VMEM((BATCHES, 4, HEAD_DIM, rows_q), F32),
                pltpu.VMEM((n_layers, n_sp, BATCHES, chips, CORES, sub, 2 * HEAD_DIM), BF16),
                pltpu.VMEM((BATCHES, chips, CORES, sub, HEAD_DIM), F32),
                pltpu.VMEM((n_sp, BATCHES, chips, CORES, sub, HEAD_DIM), BF16),
                pltpu.VMEM((model_dim, q_dim + 2 * HEAD_DIM), BF16),
                pltpu.VMEM((q_dim, model_dim), BF16),
                pltpu.VMEM((model_dim, ffn), BF16),
                pltpu.VMEM((model_dim, ffn), BF16),
                pltpu.VMEM((ffn, model_dim), BF16),
                dma((7,)),
                dma((BATCHES, 10)), dma((BATCHES,)), dma((BATCHES, 2)), dma((BATCHES, 2)), dma((BATCHES, 2)), dma((BATCHES, 3)),
                dma((BATCHES, 4)), dma((BATCHES, 4)), dma((BATCHES, 6)), dma((BATCHES, 2)), dma((BATCHES, 2, 2)),
                dma((BATCHES, n_sp - 1)), dma((n_layers, n_sp, BATCHES)), dma((BATCHES, CORES, 2)),
                dma((n_tp,)), dma((n_tp,)), dma((n_tp,)), dma((n_tp,)), dma((n_sp - 1,)), dma((n_sp,)),
            ],
            compiler_params=pltpu.CompilerParams(collective_id=0, has_side_effects=True, vmem_limit_bytes=67_000_000),
        )(hidden_in.reshape(BATCHES, sub, model_dim), tab, hot, attn_gain, mlp_gain,
          w_q, w_k, w_v, w_o, w_gate, w_up, w_down)
        cache_shape = (n_layers, n_rows, 1, HEAD_DIM)
        return out.reshape(tok_local, model_dim), k_c.reshape(cache_shape), v_c.reshape(cache_shape)

    return jax.shard_map(device_fn, mesh=mesh,
                         in_specs=(P(('dp', 'sp', 'tp'), None), tok_spec, tok_spec, P(), col_spec, col_spec, col_spec, row_spec, P(), col_spec, col_spec, row_spec),
                         out_specs=(P(('dp', 'sp', 'tp'), None), cache_spec, cache_spec), check_vma=False)
```

```python
import jax
import jax.numpy as jnp
from jax import lax
from jax.experimental import pallas as pl
from jax.experimental.pallas import tpu as pltpu
from jax.sharding import PartitionSpec as P

HEAD_DIM = 128
ROPE_BASE = 1e4
NORM_EPS = 1e-5
LOG2E = 1.4426950408889634
SCORE_EXP2 = HEAD_DIM ** -0.5 * LOG2E
NEG = -1e30
SPLIT = 2.0 ** 99
MESH = pl.DeviceIdType.MESH
F32 = jnp.float32
BF16 = jnp.bfloat16
CORES = 2
BATCHES = 2
OPP, RIGHT, LEFT, OWN = 0, 1, 2, 3


def dot(a, b):
    return jnp.dot(a, b, preferred_element_type=F32)


def make_kernel(n_layers, n_sp, n_tp, sub, model_dim, q_dim, ffn, col):
    chips = n_tp // CORES
    half = sub // 2
    unit = CORES * sub
    heads = q_dim // HEAD_DIM
    chip_rows = BATCHES * unit

    def kernel(hid, tab_own, hot_own, gain_a, gain_m, wq_h, wk_h, wv_h, wo_h, wg_h, wu_h, wd_h,
               out, k_out, v_out,
               res, gath, part, acc_rs, opp_in, nb_in, act, q_buf, m_buf, l_buf, o_buf, kv, tab, hot,
               w_qkv, w_o, w_g, w_u, w_d,
               w_sem, ag_send, ag_sib, ag_l, ag_r, ag_o, ag_sf, rs_dsend, rs_sib, rs_send, rs_opp, rs_nb, kv_send, kv_recv, c_sem, t_send, t_recv, h_send, h_recv, e_send, e_recv):
        y = lax.axis_index('sp')
        me = lax.axis_index('tp')
        x = me // CORES
        c = lax.rem(me, CORES)
        oc = 1 - c
        xl = lax.rem(x + chips - 1, chips)
        xr = lax.rem(x + 1, chips)
        xo = lax.rem(x + 2, chips)

        def unit_of(k):
            if isinstance(k, int):
                return (xo, xr, xl, x)[k]
            p, i = k // 2, lax.rem(k, 2)
            return lax.rem(x + (2 + p) * (1 - i) + (1 - p) * i, chips)
        sib = {'tp': x * CORES + oc}
        right = {'tp': xr * CORES + c}
        left = {'tp': xl * CORES + c}
        lo = pl.ds(0, half)
        hi = pl.ds(half, half)

        def rdma(src, dst, ssem, rsem, dev):
            return pltpu.make_async_remote_copy(src_ref=src, dst_ref=dst, send_sem=ssem, recv_sem=rsem,
                                                device_id=dev, device_id_type=MESH)

        def attn_weights(l):
            return [pltpu.make_async_copy(wq_h.at[l], w_qkv.at[:, pl.ds(0, q_dim)], w_sem.at[0]),
                    pltpu.make_async_copy(wk_h.at[l], w_qkv.at[:, pl.ds(q_dim, HEAD_DIM)], w_sem.at[1]),
                    pltpu.make_async_copy(wv_h.at[l], w_qkv.at[:, pl.ds(q_dim + HEAD_DIM, HEAD_DIM)], w_sem.at[2]),
                    pltpu.make_async_copy(wo_h.at[l], w_o, w_sem.at[3])]

        def mlp_weights(l):
            return [pltpu.make_async_copy(wg_h.at[l], w_g, w_sem.at[4]),
                    pltpu.make_async_copy(wu_h.at[l], w_u, w_sem.at[5]),
                    pltpu.make_async_copy(wd_h.at[l], w_d, w_sem.at[6])]

        for cp in attn_weights(0) + mlp_weights(0):
            cp.start()

        barrier = pltpu.get_barrier_semaphore()
        for t in range(1, n_tp):
            pl.semaphore_signal(barrier, inc=1, device_id={'tp': lax.rem(me + t, n_tp)}, device_id_type=MESH)
        for d in range(1, n_sp):
            pl.semaphore_signal(barrier, inc=1, device_id={'sp': lax.rem(y + d, n_sp)}, device_id_type=MESH)
        pl.semaphore_wait(barrier, n_tp - 1 + n_sp - 1)

        def ag_copies(b):
            own = gath.at[b, x, c]
            return {
                'sib': lambda: rdma(own, own, ag_send.at[b, 0], ag_sib.at[b], sib),
                'r_lo': lambda: rdma(own.at[lo], own.at[lo], ag_send.at[b, 1], ag_l.at[b, 0], right),
                'l_hi': lambda: rdma(own.at[hi], own.at[hi], ag_send.at[b, 2], ag_r.at[b, 1], left),
                'r_hi': lambda: rdma(own.at[hi], own.at[hi], ag_send.at[b, 3], ag_l.at[b, 1], right),
                'l_lo': lambda: rdma(own.at[lo], own.at[lo], ag_send.at[b, 4], ag_r.at[b, 0], left),
                'f_r': lambda: rdma(gath.at[b, xl, c, lo], gath.at[b, xl, c, lo], ag_send.at[b, 5], ag_o.at[b, 0], right),
                'f_l': lambda: rdma(gath.at[b, xr, c, hi], gath.at[b, xr, c, hi], ag_send.at[b, 6], ag_o.at[b, 1], left),
                's_l': lambda: rdma(gath.at[b, xl, c], gath.at[b, xl, c], ag_send.at[b, 7], ag_sf.at[b, LEFT], sib),
                's_r': lambda: rdma(gath.at[b, xr, c], gath.at[b, xr, c], ag_send.at[b, 8], ag_sf.at[b, RIGHT], sib),
                's_o': lambda: rdma(gath.at[b, xo, c], gath.at[b, xo, c], ag_send.at[b, 9], ag_sf.at[b, OPP], sib),
            }

        def arrived(ref, sem):
            rdma(ref, ref, ag_send.at[0, 0], sem, sib).wait_recv()

        def ag0a(b):
            cps = ag_copies(b)
            for name in ('sib', 'r_lo', 'l_hi'):
                cps[name]().start()

        def ag0b(b):
            cps = ag_copies(b)
            for name in ('r_hi', 'l_lo'):
                cps[name]().start()

        def ag1(b):
            cps = ag_copies(b)
            arrived(gath.at[b, xl, c, lo], ag_l.at[b, 0])
            cps['f_r']().start()
            arrived(gath.at[b, xr, c, hi], ag_r.at[b, 1])
            cps['f_l']().start()

        def ag2(b):
            cps = ag_copies(b)
            arrived(gath.at[b, xl, c, hi], ag_l.at[b, 1])
            cps['s_l']().start()
            arrived(gath.at[b, xr, c, lo], ag_r.at[b, 0])
            cps['s_r']().start()

        def ag3(b):
            cps = ag_copies(b)
            arrived(gath.at[b, xo, c, lo], ag_o.at[b, 0])
            arrived(gath.at[b, xo, c, hi], ag_o.at[b, 1])
            cps['s_o']().start()

        def ag_unit_ready(b, k):
            arrived(gath.at[b, unit_of(k), oc], ag_sib.at[b] if isinstance(k, int) and k == OWN else ag_sf.at[b, k])

        def ag_sent(b):
            for cp in ag_copies(b).values():
                cp().wait_send()

        def rs_pair(b, k):
            return rdma(part.at[k, oc], acc_rs.at[b, k], rs_dsend.at[b, k], rs_sib.at[b, k], sib)

        def rs_copies(b):
            return {
                'o_r': lambda: rdma(acc_rs.at[b, OPP, lo], opp_in.at[b, 0], rs_send.at[b, 0], rs_opp.at[b, 0], right),
                'o_l': lambda: rdma(acc_rs.at[b, OPP, hi], opp_in.at[b, 1], rs_send.at[b, 1], rs_opp.at[b, 1], left),
                'r_hi': lambda: rdma(acc_rs.at[b, RIGHT, hi], nb_in.at[b, 0, hi], rs_send.at[b, 2], rs_nb.at[b, 0, 1], right),
                'l_lo': lambda: rdma(acc_rs.at[b, LEFT, lo], nb_in.at[b, 1, lo], rs_send.at[b, 3], rs_nb.at[b, 1, 0], left),
                'r_lo': lambda: rdma(acc_rs.at[b, RIGHT, lo], nb_in.at[b, 0, lo], rs_send.at[b, 4], rs_nb.at[b, 0, 0], right),
                'l_hi': lambda: rdma(acc_rs.at[b, LEFT, hi], nb_in.at[b, 1, hi], rs_send.at[b, 5], rs_nb.at[b, 1, 1], left),
            }

        def pair_sum(b, k):
            cp = rs_pair(b, k)
            cp.wait_send()
            cp.wait_recv()
            acc_rs[b, k] = (acc_rs[b, k].astype(F32) + part[k, c].astype(F32)).astype(BF16)

        def rs1(b):
            pair_sum(b, OPP)
            cps = rs_copies(b)
            cps['o_r']().start()
            cps['o_l']().start()

        def rs2a(b):
            cps = rs_copies(b)
            pair_sum(b, RIGHT)
            cps['r_hi']().start()
            pair_sum(b, LEFT)
            cps['l_lo']().start()
            pair_sum(b, OWN)

        def rs2b(b):
            cps = rs_copies(b)
            cps['o_r']().wait_recv()
            acc_rs[b, RIGHT, lo] = (acc_rs[b, RIGHT, lo].astype(F32) + opp_in[b, 0].astype(F32)).astype(BF16)
            cps['r_lo']().start()
            cps['o_l']().wait_recv()
            acc_rs[b, LEFT, hi] = (acc_rs[b, LEFT, hi].astype(F32) + opp_in[b, 1].astype(F32)).astype(BF16)
            cps['l_hi']().start()

        def fin(b):
            cps = rs_copies(b)
            for name in ('r_hi', 'l_lo', 'r_lo', 'l_hi'):
                cps[name]().wait_recv()
            for cp in cps.values():
                cp().wait_send()
            total = (acc_rs[b, OWN].astype(F32) + nb_in[b, 0].astype(F32) + nb_in[b, 1].astype(F32)).astype(BF16)
            res[b] = (res[b].astype(F32) + total.astype(F32)).astype(BF16)

        def norm(b, gain):
            h = res[b].astype(F32)
            inv = lax.rsqrt(jnp.mean(h * h, axis=-1, keepdims=True) + NORM_EPS)
            gath[b, x, c] = (h * inv * gain).astype(BF16)

        def gain_row(ref, l):
            rows = ref[...].astype(F32)
            row = rows[0:1]
            for i in range(1, n_layers):
                row = jnp.where(l == i, rows[i:i + 1], row)
            return row

        def store_part(k, lhs, w, n):
            cols = pl.ds(n * col if isinstance(n, int) else pl.multiple_of(n * col, col), col)
            r = dot(lhs, w[:, cols]).astype(BF16)
            part[k, :, :, cols] = r.reshape(CORES, sub, col)

        def rope(v, cos_v, sin_v):
            return v * cos_v + pltpu.roll(v, HEAD_DIM // 2, 1) * sin_v

        def qkv(l, b, k):
            ag_unit_ready(b, k)
            u = unit_of(k)
            n = gath[b, u].reshape(unit, model_dim)
            packed = tab[b, u].reshape(unit, HEAD_DIM)
            swapped = pltpu.roll(packed, HEAD_DIM // 2, 1)
            first = lax.broadcasted_iota(jnp.int32, (unit, HEAD_DIM), 1) < HEAD_DIM // 2
            cos_v = jnp.where(first, packed, swapped)
            sin_v = jnp.where(first, -swapped, packed)
            away = ((hot[y, b, u].reshape(unit, HEAD_DIM).astype(F32) - 1.0) * SPLIT).astype(BF16)
            for h0 in range(0, heads + 2, 2):
                width = min(2, heads + 2 - h0) * HEAD_DIM
                r = dot(n, w_qkv[:, pl.ds(h0 * HEAD_DIM, width)])
                for h in range(h0, min(h0 + 2, heads + 2)):
                    v = r[:, (h - h0) * HEAD_DIM:(h - h0 + 1) * HEAD_DIM]
                    if h < heads:
                        q_buf[b, k, h, :, pl.ds(0, HEAD_DIM)] = rope(v, cos_v, sin_v).astype(BF16)
                        q_buf[b, k, h, :, pl.ds(HEAD_DIM, HEAD_DIM)] = away
                    elif h == heads:
                        kv[l, y, b, u, :, :, pl.ds(0, HEAD_DIM)] = rope(v, cos_v, sin_v).astype(BF16).reshape(CORES, sub, HEAD_DIM)
                    else:
                        kv[l, y, b, u, :, :, pl.ds(HEAD_DIM, HEAD_DIM)] = v.astype(BF16).reshape(CORES, sub, HEAD_DIM)
            m_buf[b, k] = jnp.full(m_buf.shape[2:], NEG, F32)
            l_buf[b, k] = jnp.zeros(l_buf.shape[2:], F32)
            o_buf[b, k] = jnp.zeros(o_buf.shape[2:], F32)
            for d in range(1, n_sp):
                @pl.when(y + d < n_sp)
                def _():
                    kv_copy(b, l, kv.at[l, y, b, u], d).start()

        def kv_copy(b, l, ref, d):
            return rdma(ref, ref, kv_send.at[b, d - 1], kv_recv.at[l, y, b], {'sp': lax.min(y + d, n_sp - 1)})

        def cache_copies(l):
            cps = []
            for b in range(BATCHES):
                for core in range(CORES):
                    for i, ref in enumerate((k_out, v_out)):
                        cps.append(pltpu.make_async_copy(kv.at[l, y, b, :, core, :, pl.ds(i * HEAD_DIM, HEAD_DIM)],
                                                         ref.at[l, :, core, b], c_sem.at[b, core, i]))
            return cps

        def flash(b, ks, block, marks, masks=None):
            n_keys = block.shape[0]
            keys = jnp.concatenate([block[:, :HEAD_DIM], marks], axis=1)
            vals = block[:, HEAD_DIM:]
            scores = [lax.dot_general(keys, q_buf[b, k].reshape(heads * unit, 2 * HEAD_DIM), (((1,), (1,)), ((), ())),
                                      preferred_element_type=F32) for k in ks]
            for i, k in enumerate(ks):
                s = scores[i]
                if masks is not None:
                    s = jnp.where(masks[i], s, NEG)
                m_old = m_buf[b, k]
                m_new = jnp.maximum(m_old, jnp.max(s, axis=0, keepdims=True))
                alpha = jnp.exp2((m_old - m_new) * SCORE_EXP2)
                p = jnp.exp2((s - m_new[0:1]) * SCORE_EXP2)
                m_buf[b, k] = m_new
                l_buf[b, k] = l_buf[b, k] * alpha + jnp.sum(p.reshape(n_keys // 8, 8, heads * unit), axis=0)
                o_buf[b, k] = o_buf[b, k] * alpha[0:1] + lax.dot_general(vals, p.astype(BF16), (((0,), (0,)), ((), ())),
                                                                         preferred_element_type=F32)

        def row_block(l, r, kb):
            return kv[l, r, kb].reshape(chips * unit, 2 * HEAD_DIM), hot[r, kb].reshape(chips * unit, HEAD_DIM)

        def whole_row(l, r):
            n = BATCHES * chips * unit
            return kv[l, r].reshape(n, 2 * HEAD_DIM), hot[r].reshape(n, HEAD_DIM)

        def attn_below(l, b, ks, a0, a1, b0, b1):
            n_a = a1 - a0

            def step(n, carry):
                kb = jnp.where(n >= n_a, 1, 0)
                flash(b, ks, *row_block(l, n + a0 + kb * (b0 - n_a - a0), kb))
                return carry

            lax.fori_loop(0, n_a + b1 - b0, step, 0)

        def attn_below_rows(l, b, ks):
            def step(r, carry):
                flash(b, ks, *whole_row(l, r))
                return carry

            lax.fori_loop(0, y, step, 0)

        def kv_ready(l, kb, first, last):
            for r in range(n_sp - 1):
                @pl.when(jnp.logical_and(r >= first, r < last))
                def _():
                    rdma(kv.at[l, r, kb], kv.at[l, r, kb], kv_send.at[0, 0], kv_recv.at[l, r, kb], sib).wait_recv()

        def attn_own(l, b, ks, kb=None):
            n_keys = chips * unit * (BATCHES if kb is None else 1)
            key = lax.broadcasted_iota(jnp.int32, (n_keys, unit), 0)
            qry = lax.broadcasted_iota(jnp.int32, (n_keys, unit), 1)
            k_batch = key // (chips * unit) if kb is None else kb
            k_tok = lax.rem(key, chips * unit) // sub * (BATCHES * sub) + lax.rem(key, sub) + k_batch * sub
            ahead = qry // sub * (BATCHES * sub) + lax.rem(qry, sub) + b * sub - k_tok
            masks = [jnp.concatenate([ahead >= -unit_of(k) * chip_rows] * heads, axis=1) for k in ks]
            flash(b, ks, *(whole_row(l, y) if kb is None else row_block(l, y, kb)), masks)

        def attn_out(b, p):
            def one(i, carry):
                k = 2 * p + i
                o = o_buf[b, k] * (1.0 / jnp.sum(l_buf[b, k], axis=0, keepdims=True))
                o = jnp.concatenate([o[:, h * unit:(h + 1) * unit].T.astype(BF16) for h in range(heads)], axis=1)
                for n in range(model_dim // col):
                    store_part(k, o, w_o, n)
                rs_pair(b, k).start()
                return carry

            lax.fori_loop(0, 2, one, 0)

        ffn_col = min(1024, ffn)

        def gate_up(b, k):
            ag_unit_ready(b, k)
            n = gath[b, unit_of(k)].reshape(unit, model_dim)

            def step(j, carry):
                cols = pl.ds(j * ffn_col, ffn_col)
                g = dot(n, w_g[:, cols])
                act[b, k, :, cols] = (g * jax.nn.sigmoid(g) * dot(n, w_u[:, cols])).astype(BF16)
                return carry

            for j in range(ffn // ffn_col):
                step(j, 0)

        def down(b, p):
            def one(i, carry):
                k = 2 * p + i
                for n in range(model_dim // col):
                    store_part(k, act[b, k], w_d, n)
                rs_pair(b, k).start()
                return carry

            lax.fori_loop(0, 2, one, 0)

        def sides(fn, b):
            def one(i, carry):
                fn(b, LEFT - i)
                return carry

            lax.fori_loop(0, 2, one, 0)

        A, B = 0, 1
        res[...] = hid[...]
        norm(A, gain_row(gain_a, 0))
        ag0a(A)
        tab[:, x, c] = tab_own[...]
        hot[y, :, x, c] = hot_own[...]

        def peer_copies(t, src):
            to = {'tp': lax.rem(me + t, n_tp)}
            return (rdma(tab_own, tab.at[:, src // CORES, lax.rem(src, CORES)], t_send.at[t], t_recv.at[src], to),
                    rdma(hot_own, hot.at[y, :, src // CORES, lax.rem(src, CORES)], h_send.at[t], h_recv.at[src], to))

        def hot_copy(d):
            return rdma(hot.at[y], hot.at[y], e_send.at[d - 1], e_recv.at[y], {'sp': lax.min(y + d, n_sp - 1)})

        for t in range(1, n_tp):
            for cp in peer_copies(t, me):
                cp.start()
        for t in range(1, n_tp):
            for cp in peer_copies(t, lax.rem(me + t, n_tp)):
                cp.wait_recv()
        for d in range(1, n_sp):
            @pl.when(y + d < n_sp)
            def _():
                hot_copy(d).start()

        def layer(l, carry):
            more = l + 1 < n_layers
            nxt = lax.min(l + 1, n_layers - 1)
            for cp in attn_weights(l)[:3]:
                cp.wait()
            def qkv_l(b, k):
                qkv(l, b, k)

            qkv(l, A, OWN)

            @pl.when(l > 0)
            def _():
                rs2b(B)
            ag0b(A)
            ag1(A)

            @pl.when(l > 0)
            def _():
                fin(B)
            norm(B, gain_row(gain_a, l))
            ag0a(B)
            ag2(A)
            ag0b(B)
            sides(qkv_l, A)
            ahead = lax.max(y - 1, 0)
            a_soon = jnp.where(l > 0, ahead, 0)
            b_soon = jnp.where(l > 1, ahead, 0)
            b_early = jnp.where(l > 0, ahead, 0)

            def early(e, carry):
                @pl.when(e == 1)
                def _():
                    ag3(A)
                    qkv(l, B, OWN)
                    ag1(B)
                    qkv(l, A, OPP)

                    @pl.when(l == 0)
                    def _():
                        for r in range(n_sp - 1):
                            @pl.when(r < y)
                            def _():
                                rdma(hot.at[r], hot.at[r], e_send.at[0], e_recv.at[r], sib).wait_recv()

                a0, a1 = jnp.where(e == 0, 0, a_soon), jnp.where(e == 0, a_soon, y)
                b0, b1 = jnp.where(e == 0, 0, b_soon), jnp.where(e == 0, b_soon, b_early)
                kv_ready(l, A, a0, a1)
                kv_ready(l, B, b0, b1)
                attn_below(l, A, (RIGHT, LEFT, OWN), a0, a1, b0, b1)
                return carry

            lax.fori_loop(0, 2, early, 0)
            attn_below(l, A, (OPP,), 0, y, 0, b_early)
            attn_own(l, A, (OPP, RIGHT, LEFT, OWN), A)
            ag2(B)
            sides(qkv_l, B)
            ag3(B)
            attn_weights(l)[3].wait()
            ag_sent(A)
            qkv(l, B, OPP)
            for cp in cache_copies(l):
                cp.start()

            def late_a(p, carry):
                ks = (2 * p, 2 * p + 1)
                attn_own(l, A, ks, B)

                @pl.when(p == 0)
                def _():
                    kv_ready(l, B, b_early, y)
                attn_below(l, A, ks, 0, 0, b_early, y)
                attn_out(A, p)

                @pl.when(p == 0)
                def _():
                    rs1(A)
                return carry

            lax.fori_loop(0, 2, late_a, 0)
            rs2a(A)
            ag_sent(B)

            def late_b(p, carry):
                ks = (2 * p, 2 * p + 1)
                attn_own(l, B, ks)

                @pl.when(p == 0)
                def _():
                    rs2b(A)
                attn_below_rows(l, B, ks)
                attn_out(B, p)

                @pl.when(p == 0)
                def _():
                    rs1(B)
                    fin(A)
                    norm(A, gain_row(gain_m, l))
                    ag0a(A)
                return carry

            lax.fori_loop(0, 2, late_b, 0)

            @pl.when(more)
            def _():
                for cp in attn_weights(nxt):
                    cp.start()
            rs2a(B)
            for cp in mlp_weights(l)[:2]:
                cp.wait()
            gate_up(A, OWN)
            rs2b(B)
            ag0b(A)
            ag1(A)
            fin(B)
            norm(B, gain_row(gain_m, l))
            ag0a(B)
            ag2(A)
            ag0b(B)
            sides(gate_up, A)
            ag3(A)
            gate_up(B, OWN)
            ag1(B)
            gate_up(A, OPP)
            mlp_weights(l)[2].wait()
            ag_sent(A)
            down(A, 0)
            rs1(A)
            down(A, 1)
            ag2(B)

            def two(i, carry):
                gate_up(B, RIGHT - i)

                @pl.when(i == 0)
                def _():
                    rs2a(A)
                    ag3(B)
                return carry

            lax.fori_loop(0, 2, two, 0)
            ag_sent(B)
            down(B, 0)
            rs2b(A)
            rs1(B)
            gate_up(B, LEFT)
            down(B, 1)

            @pl.when(more)
            def _():
                for cp in mlp_weights(nxt):
                    cp.start()
            rs2a(B)
            fin(A)

            @pl.when(more)
            def _():
                norm(A, gain_row(gain_a, nxt))
                ag0a(A)
            for cp in cache_copies(l):
                cp.wait()
            for d in range(1, n_sp):
                @pl.when(y + d < n_sp)
                def _():
                    for b in range(BATCHES):
                        kv_copy(b, l, kv.at[l, y, b], d).wait_send()
            return carry

        lax.fori_loop(0, n_layers, layer, 0)
        rs2b(B)
        fin(B)
        out[...] = res[...]
        for t in range(1, n_tp):
            for cp in peer_copies(t, me):
                cp.wait_send()
        for d in range(1, n_sp):
            @pl.when(y + d < n_sp)
            def _():
                hot_copy(d).wait_send()

    return kernel


def place(*refs):
    n = (len(refs) - 2) // 3
    src, dst, buf, sem_in, sem_out = refs[:n], refs[n:2 * n], refs[2 * n:3 * n], refs[-2], refs[-1]
    ins = [pltpu.make_async_copy(src[i], buf[i], sem_in.at[i]) for i in range(n)]
    outs = [pltpu.make_async_copy(buf[i], dst[i], sem_out.at[i]) for i in range(n)]
    for cp in ins:
        cp.start()
    for i in range(n):
        ins[i].wait()
        outs[i].start()
    for cp in outs:
        cp.wait()


def solution(mesh):
    n_sp, n_tp = mesh.shape['sp'], mesh.shape['tp']
    chips = n_tp // CORES
    tok_spec = P(('dp', 'sp', 'tp'))
    col_spec = P(None, None, 'tp')
    row_spec = P(None, 'tp', None)
    cache_spec = P(None, ('dp', 'sp'), 'tp', None)

    def device_fn(hidden_in, segment_ids, positions, attn_gain, w_q, w_k, w_v, w_o, mlp_gain, w_gate, w_up, w_down):
        tok_local, model_dim = hidden_in.shape
        n_layers, _, q_dim = w_q.shape
        ffn = w_gate.shape[2]
        sub = tok_local // BATCHES
        unit = CORES * sub
        n_rows = tok_local * n_tp
        heads = q_dim // HEAD_DIM
        col = min(1536, model_dim)

        half_dim = HEAD_DIM // 2
        inv_freq = ROPE_BASE ** (-jnp.arange(half_dim, dtype=F32) / half_dim)
        angles = positions.reshape(BATCHES, sub, 1).astype(F32) * inv_freq
        tab = jnp.concatenate([jnp.cos(angles), jnp.sin(angles)], axis=-1)
        hot = (segment_ids.reshape(BATCHES, sub, 1) == jnp.arange(HEAD_DIM)).astype(BF16)

        vmem = pl.BlockSpec(memory_space=pltpu.VMEM)
        hbm = pl.BlockSpec(memory_space=pl.ANY)
        dma = pltpu.SemaphoreType.DMA
        rows_q = heads * unit
        cache = jax.ShapeDtypeStruct((n_layers, chips, CORES, BATCHES, sub, HEAD_DIM), BF16)
        out, k_c, v_c = pl.pallas_call(
            make_kernel(n_layers, n_sp, n_tp, sub, model_dim, q_dim, ffn, col),
            name='decoder_stack',
            out_shape=(jax.ShapeDtypeStruct((BATCHES, sub, model_dim), BF16), cache, cache),
            in_specs=[vmem] * 5 + [hbm] * 7,
            out_specs=(vmem, hbm, hbm),
            scratch_shapes=[
                pltpu.VMEM((BATCHES, sub, model_dim), BF16),
                pltpu.VMEM((BATCHES, chips, CORES, sub, model_dim), BF16),
                pltpu.VMEM((4, CORES, sub, model_dim), BF16),
                pltpu.VMEM((BATCHES, 4, sub, model_dim), BF16),
                pltpu.VMEM((BATCHES, 2, sub // 2, model_dim), BF16),
                pltpu.VMEM((BATCHES, 2, sub, model_dim), BF16),
                pltpu.VMEM((BATCHES, 4, unit, ffn), BF16),
                pltpu.VMEM((BATCHES, 4, heads, unit, 2 * HEAD_DIM), BF16),
                pltpu.VMEM((BATCHES, 4, 8, rows_q), F32),
                pltpu.VMEM((BATCHES, 4, 8, rows_q), F32),
                pltpu.VMEM((BATCHES, 4, HEAD_DIM, rows_q), F32),
                pltpu.VMEM((n_layers, n_sp, BATCHES, chips, CORES, sub, 2 * HEAD_DIM), BF16),
                pltpu.VMEM((BATCHES, chips, CORES, sub, HEAD_DIM), F32),
                pltpu.VMEM((n_sp, BATCHES, chips, CORES, sub, HEAD_DIM), BF16),
                pltpu.VMEM((model_dim, q_dim + 2 * HEAD_DIM), BF16),
                pltpu.VMEM((q_dim, model_dim), BF16),
                pltpu.VMEM((model_dim, ffn), BF16),
                pltpu.VMEM((model_dim, ffn), BF16),
                pltpu.VMEM((ffn, model_dim), BF16),
                dma((7,)),
                dma((BATCHES, 10)), dma((BATCHES,)), dma((BATCHES, 2)), dma((BATCHES, 2)), dma((BATCHES, 2)), dma((BATCHES, 3)),
                dma((BATCHES, 4)), dma((BATCHES, 4)), dma((BATCHES, 6)), dma((BATCHES, 2)), dma((BATCHES, 2, 2)),
                dma((BATCHES, n_sp - 1)), dma((n_layers, n_sp, BATCHES)), dma((BATCHES, CORES, 2)),
                dma((n_tp,)), dma((n_tp,)), dma((n_tp,)), dma((n_tp,)), dma((n_sp - 1,)), dma((n_sp,)),
            ],
            compiler_params=pltpu.CompilerParams(collective_id=0, has_side_effects=True, vmem_limit_bytes=67_000_000),
        )(hidden_in.reshape(BATCHES, sub, model_dim), tab, hot, attn_gain, mlp_gain,
          w_q, w_k, w_v, w_o, w_gate, w_up, w_down)
        results = [out, k_c, v_c]
        out, k_c, v_c = pl.pallas_call(
            place,
            name='place_results',
            out_shape=[jax.ShapeDtypeStruct(r.shape, r.dtype) for r in results],
            in_specs=[hbm] * 3,
            out_specs=[hbm] * 3,
            scratch_shapes=[pltpu.VMEM(r.shape, r.dtype) for r in results] + [dma((3,)), dma((3,))],
        )(*results)
        cache_shape = (n_layers, n_rows, 1, HEAD_DIM)
        return out.reshape(tok_local, model_dim), k_c.reshape(cache_shape), v_c.reshape(cache_shape)

    return jax.shard_map(device_fn, mesh=mesh,
                         in_specs=(P(('dp', 'sp', 'tp'), None), tok_spec, tok_spec, P(), col_spec, col_spec, col_spec, row_spec, P(), col_spec, col_spec, row_spec),
                         out_specs=(P(('dp', 'sp', 'tp'), None), cache_spec, cache_spec), check_vma=False)
```
